256 devices in a mesh: dp: 16 (over x, z_hi, core), seq: 16 (over z_lo, y).
Axes of the slice: x: 4, y: 4, z: 8 (z_hi: 2, z_lo: 4; z = z_hi * 4 + z_lo), core: 2. Of those that a mesh axis runs over, the one named last changes fastest.
Arguments:
- tokens: bfloat16 [32, 2304, 1280], P('dp', 'seq'), may hold values from -60 to 60
- pre_gain: float32 [1280], replicated, may hold values from 0.5 to 1.5
- pre_shift: float32 [1280], replicated, may hold values from -3 to 3
- w_qkv: bfloat16 [1280, 3840], P('dp'), may hold values from -4 to 4
- qkv_bias: float32 [3840], replicated, may hold values from -3 to 3
- w_out: bfloat16 [1280, 1280], P('dp'), may hold values from -0.15625 to 0.15625
- out_bias: float32 [1280], replicated, may hold values from -3 to 3
- mlp_gain: float32 [1280], replicated, may hold values from 0.5 to 1.5
- mlp_shift: float32 [1280], replicated, may hold values from -3 to 3
- w_up: bfloat16 [1280, 2560], P('dp'), may hold values from -0.15625 to 0.15625
- up_bias: float32 [2560], replicated, may hold values from -3 to 3
- w_down: bfloat16 [2560, 1280], P('dp'), may hold values from -0.125 to 0.125
- down_bias: float32 [1280], replicated, may hold values from -3 to 3
Outputs:
- layer_out: bfloat16 [32, 2304, 1280], P('dp', 'seq')
The draws below stay inside these ranges and needn't reach their ends.
All inputs are finite; a program needn't handle non-finite values.
Results may differ from the reference program's by a relative error of at most 0.0039.
Values may be sent and summed in bfloat16 or wider, within the bound.
No kernel may reach another device: no remote copies, remote signals or barrier semaphores. Data moves between devices by JAX's collectives and lax.ppermute only.
A program may use at most 128 MiB of HBM per device.

```python
import math
import jax
import jax.numpy as jnp
from jax import lax

D = 1280
HEADS = 16
HEAD_DIM = 80
FF = 2560
IMAGES = 32
SEQ_LEN = 2304


def draw_tokens(key, part):
    subkeys = jax.random.split(jax.random.fold_in(key, 21), 4)
    shape = (IMAGES, SEQ_LEN, D)
    base = jax.random.normal(subkeys[0], shape, jnp.float32)
    row_scale = jnp.exp(jax.random.uniform(subkeys[2], (IMAGES, SEQ_LEN, 1), jnp.float32, math.log(0.4), math.log(4.0)))
    col_scale = jnp.exp(jax.random.uniform(subkeys[3], (1, 1, D), jnp.float32, math.log(0.4), math.log(4.0)))
    values = base * row_scale * col_scale
    return jnp.clip(values, -60.0, 60.0).astype(jnp.bfloat16)


def draw_w_qkv(key, part):
    subkey = jax.random.fold_in(key, 33)
    shape = (D, 3 * D)
    values = jnp.clip(jax.random.normal(subkey, shape, jnp.float32), -6.0, 6.0) / math.sqrt(D)
    return values.astype(jnp.bfloat16)


def block_levels(stream_key, extent, cuts, smallest, top_value):
    def one(axis_at, blocks):
        steps = jax.random.uniform(jax.random.fold_in(jax.random.fold_in(stream_key, 6), axis_at), (blocks,), jnp.float32, smallest / len(cuts), top_value / len(cuts))
        return jnp.repeat(jnp.exp(steps), extent[axis_at] // blocks).reshape((-1,) + (1,) * (len(extent) - axis_at - 1))

    level = one(*cuts[0])
    for cut in cuts[1:]:
        level = level * one(*cut)
    return level


def bell_draw(stream_key, extent, deviation, bound, cuts=(), held_as=jnp.bfloat16):
    array = jax.random.normal(stream_key, extent, jnp.float32) * deviation
    if len(cuts) > 0:
        array = block_levels(stream_key, extent, cuts, -0.22, 0.18) * array
    return jnp.clip(array, min=-bound, max=bound).astype(held_as)


def setup_inputs(seed: int = 0) -> dict:
    key_of = jax.random.split(jax.random.key(seed), 14)
    return {
        "tokens": draw_tokens(jax.random.fold_in(key_of[13], 71), 0),
        "pre_gain": jnp.clip(1.0 + 0.1 * jax.random.normal(key_of[1], (D,), jnp.float32), 0.5, 1.5),
        "pre_shift": bell_draw(key_of[2], (D,), 0.5, 3.0, (), jnp.float32),
        "w_qkv": draw_w_qkv(jax.random.fold_in(key_of[13], 71), 0),
        "qkv_bias": bell_draw(key_of[4], (3 * D,), 0.5, 3.0, (), jnp.float32),
        "w_out": bell_draw(key_of[5], (D, D), D ** -0.5, 0.15625, ((0, 16),)),
        "out_bias": bell_draw(key_of[6], (D,), 0.5, 3.0, (), jnp.float32),
        "mlp_gain": jnp.clip(1.0 + 0.1 * jax.random.normal(key_of[7], (D,), jnp.float32), 0.5, 1.5),
        "mlp_shift": bell_draw(key_of[8], (D,), 0.5, 3.0, (), jnp.float32),
        "w_up": bell_draw(key_of[9], (D, FF), D ** -0.5, 0.15625, ((0, 16),)),
        "up_bias": bell_draw(key_of[10], (FF,), 0.5, 3.0, (), jnp.float32),
        "w_down": bell_draw(key_of[11], (FF, D), FF ** -0.5, 0.125, ((0, 16),)),
        "down_bias": bell_draw(key_of[12], (D,), 0.5, 3.0, (), jnp.float32),
    }


EPSILON = 1e-05

def normalize(features, gain, shift):
    average = lax.optimization_barrier(jnp.mean(features, axis=-1, keepdims=True))
    centered = features - average
    spread = lax.optimization_barrier(jnp.mean(centered * centered, axis=-1, keepdims=True))
    return centered * lax.rsqrt(spread + EPSILON) * gain + shift

def attend_head(packed_head):
    queries = packed_head[:, :HEAD_DIM]
    key_rows = packed_head[:, HEAD_DIM:2 * HEAD_DIM]
    value_rows = packed_head[:, 2 * HEAD_DIM:]
    scores = jnp.dot(queries, key_rows.T, preferred_element_type=jnp.float32) * (1.0 / math.sqrt(HEAD_DIM))
    highest = lax.optimization_barrier(jnp.max(scores, axis=-1, keepdims=True))
    weights = jnp.exp(scores - highest)
    probs = (weights / lax.optimization_barrier(jnp.sum(weights, axis=-1, keepdims=True))).astype(jnp.bfloat16)
    return jnp.dot(probs, value_rows, preferred_element_type=jnp.float32).astype(jnp.bfloat16)

def reference(tokens, pre_gain, pre_shift, w_qkv, qkv_bias, w_out, out_bias, mlp_gain, mlp_shift, w_up, up_bias, w_down, down_bias):

    def one_picture(picture):
        residual = picture.astype(jnp.float32)
        normed = normalize(residual, pre_gain, pre_shift).astype(jnp.bfloat16)
        packed = (jnp.dot(normed, w_qkv, preferred_element_type=jnp.float32) + qkv_bias).astype(jnp.bfloat16)
        per_head = packed.reshape(SEQ_LEN, HEADS, 3 * HEAD_DIM).transpose(1, 0, 2)
        context = lax.map(attend_head, per_head)
        context = context.transpose(1, 0, 2).reshape(SEQ_LEN, D)
        middle = residual + jnp.dot(context, w_out, preferred_element_type=jnp.float32) + out_bias
        normed_mlp = normalize(middle, mlp_gain, mlp_shift).astype(jnp.bfloat16)
        lifted = jnp.dot(normed_mlp, w_up, preferred_element_type=jnp.float32) + up_bias
        hidden = jax.nn.gelu(lifted, approximate=False).astype(jnp.bfloat16)
        lowered = jnp.dot(hidden, w_down, preferred_element_type=jnp.float32)
        return (middle + lowered + down_bias).astype(jnp.bfloat16)
    return lax.map(one_picture, tokens)
```

```python
import math

import jax
import jax.numpy as jnp
from jax import lax
from jax.experimental import pallas as pl
from jax.experimental.pallas import tpu as pltpu
from jax.sharding import Mesh
from jax.sharding import PartitionSpec as P

HEADS = 16
HEAD_DIM = 80
EPSILON = 1e-05
LANES = 128
SLOT = 2 * LANES
FIRST = LANES - HEAD_DIM
QUARTER = 112
BF = jnp.bfloat16
F32 = jnp.float32
ANY = pl.BlockSpec(memory_space=pl.ANY)
SMEM = pl.BlockSpec(memory_space=pltpu.SMEM)
VMEM = pl.BlockSpec(memory_space=pltpu.VMEM)


def shift(a, axis, by, size):
    return lax.ppermute(a, axis, [(i, (i + by) % size) for i in range(size)])


def normalize(features, gain, shift_by):
    average = jnp.mean(features, axis=-1, keepdims=True)
    centered = features - average
    spread = jnp.mean(centered * centered, axis=-1, keepdims=True)
    return centered * lax.rsqrt(spread + EPSILON) * gain + shift_by


def run_copies(copies):
    for when, copy in copies:
        if when is None:
            copy.start()
        else:
            pl.when(when)(copy.start)


def wait_copies(copies):
    for when, copy in copies:
        if when is None:
            copy.wait()
        else:
            pl.when(when)(copy.wait)


def aligned(i, m):
    return pl.multiple_of(i * m, m)


def project_kernel(pieces, n_tok, pos, *refs):
    tok = refs[:n_tok]
    wts = refs[n_tok : n_tok + len(pieces)]
    gain, shift_by, bias, out, tok_s, nrm_s, w_s, sem_t, sem_w = refs[n_tok + len(pieces) :]
    x, zh, c, zl = pos[0], pos[1], pos[2], pos[3]
    rows = tok[0].shape[0]
    moves = [(None, pltpu.make_async_copy(tok[0], tok_s.at[pl.ds(aligned(zl, rows), rows)], sem_t.at[0]))]
    for n in (1, 2, 3):
        up = pltpu.make_async_copy(tok[n], tok_s.at[pl.ds(aligned(jnp.maximum(zl - n, 0), rows), rows)], sem_t.at[n])
        down = pltpu.make_async_copy(tok[3 + n], tok_s.at[pl.ds(aligned(jnp.minimum(zl + n, 3), rows), rows)], sem_t.at[3 + n])
        moves.append((zl >= n, up))
        moves.append((zl + n <= 3, down))
    run_copies(moves)
    w_moves = []
    for i, (dx, oz, oc, row0, count, src0) in enumerate(pieces):
        d = ((x + 4 - dx) % 4) * 4 + ((zh + oz) % 2) * 2 + (c + oc) % 2
        dst = w_s.at[pl.ds(aligned(d, HEAD_DIM) + row0, count)]
        w_moves.append((None, pltpu.make_async_copy(wts[i].at[pl.ds(src0, count)], dst, sem_w.at[i])))
    run_copies(w_moves)
    wait_copies(moves)
    nrm_s[...] = normalize(tok_s[...].astype(F32), gain[...], shift_by[...]).astype(BF)
    wait_copies(w_moves)
    for k in range(4):
        cols = slice(k * SLOT, (k + 1) * SLOT)
        acc = jnp.dot(nrm_s[...], w_s[:, cols], preferred_element_type=F32)
        out[k] = (acc + bias[:, cols]).astype(BF)


def attend_kernel(block_rows, pos, b0, b1, b2, b3, out, s_ref, sem):
    y = pos[4]
    rows = b0.shape[0]
    part = rows // 4
    copies = [
        (None, pltpu.make_async_copy(b, s_ref.at[pl.ds(k * rows, rows)], sem.at[k]))
        for k, b in enumerate((b0, b1, b2, b3))
    ]
    run_copies(copies)
    wait_copies(copies)
    factor = math.log2(math.e) / math.sqrt(HEAD_DIM)
    lane = lax.broadcasted_iota(jnp.int32, (block_rows, LANES), 1)
    for r in range(4 * rows // block_rows):
        q = s_ref[r * block_rows : (r + 1) * block_rows, :LANES]
        q = jnp.where(lane < HEAD_DIM, q, jnp.zeros_like(q))
        scores = lax.dot_general(q, s_ref[:, LANES:], (((1,), (1,)), ((), ())), preferred_element_type=F32)
        highest = jnp.max(scores, axis=-1, keepdims=True)
        weights = jnp.exp2((scores - highest) * factor).astype(BF)
        mixed = jnp.dot(weights, s_ref[...], preferred_element_type=F32)
        total = mixed[:, 240:241]
        first = pltpu.roll(mixed[:, :LANES], LANES - HEAD_DIM, 1)
        second = pltpu.roll(mixed[:, LANES:], LANES - (HEAD_DIM - FIRST), 1)
        joined = jnp.where(lane < FIRST, first, second)
        joined = jnp.where(lane < HEAD_DIM, joined / total, 0.0).astype(BF)
        for p in range(block_rows // part):
            g = r * (block_rows // part) + p
            k, j = g // 4, g % 4
            out[j * 4 + (y + 4 - k) % 4] = joined[p * part : (p + 1) * part]


def finish_kernel(own, other, n_own, n_other, pos, c0, c1, tokens, *refs):
    own_w = refs[:n_own]
    other_w = refs[n_own : n_own + n_other]
    vectors = refs[n_own + n_other : n_own + n_other + 6]
    out_bias, mlp_gain, mlp_shift, up_bias, down_bias = vectors[:5]
    out = vectors[5]
    w_s, mid_s, nrm_s, hid_s, sem = refs[n_own + n_other + 6 :]
    x, zh, c, y = pos[0], pos[1], pos[2], pos[4]
    n = 0
    moves = []
    for i, (dx, oz, oc, row0, count, src0) in enumerate(own):
        d = ((x + 4 - dx) % 4) * 4 + ((zh + oz) % 2) * 2 + (c + oc) % 2
        moves.append((None, pltpu.make_async_copy(own_w[i].at[pl.ds(src0, count)], w_s.at[d, pl.ds(row0, count)], sem.at[n])))
        n += 1
    for i, (dx, oz, oc, quarter0, quarters) in enumerate(other):
        d = ((x + 4 - dx) % 4) * 4 + ((zh + oz) % 2) * 2 + (c + oc) % 2
        for k in range(quarters):
            q = (y + 4 - quarter0 - k) % 4
            src = other_w[i].at[pl.ds(k * QUARTER, QUARTER)]
            moves.append((None, pltpu.make_async_copy(src, w_s.at[d, pl.ds(aligned(q, QUARTER), QUARTER)], sem.at[n])))
            n += 1
    run_copies(moves)
    rows = tokens.shape[1]
    wait_copies(moves)
    for i, ctx in enumerate((c0, c1)):
        acc = tokens[i].astype(F32)
        for h in range(HEADS):
            acc = acc + jnp.dot(ctx[h], w_s[h, :LANES, :], preferred_element_type=F32)
        acc = acc + out_bias[...]
        mid_s[i * rows : (i + 1) * rows] = acc
        nrm_s[i * rows : (i + 1) * rows] = normalize(acc, mlp_gain[...], mlp_shift[...]).astype(BF)
    width = mid_s.shape[1]
    for half in range(2):
        for n0 in range(0, width, SLOT):
            w = w_s[:, HEAD_DIM * (1 + half) : HEAD_DIM * (2 + half), n0 : n0 + SLOT].reshape(width, SLOT)
            at = half * width + n0
            lifted = jnp.dot(nrm_s[...], w, preferred_element_type=F32) + up_bias[:, at : at + SLOT]
            hid_s[:, at : at + SLOT] = (0.5 * lifted * (1.0 + lax.erf(lifted * math.sqrt(0.5)))).astype(BF)
    for n0 in range(0, width, SLOT):
        w = w_s[:, HEAD_DIM * 3 : HEAD_DIM * 5, n0 : n0 + SLOT].reshape(2 * width, SLOT)
        lowered = jnp.dot(hid_s[...], w, preferred_element_type=F32)
        result = (mid_s[:, n0 : n0 + SLOT] + lowered + down_bias[:, n0 : n0 + SLOT]).astype(BF)
        for i in range(2):
            out[i, :, n0 : n0 + SLOT] = result[i * rows : (i + 1) * rows]


def ring_gather(a, cut):
    forth = shift(a, "x", 1, 4)
    back = shift(a, "x", -1, 4)
    far_a = shift(forth[:cut], "x", 1, 4)
    far_b = shift(back[cut:], "x", -1, 4)
    n = a.shape[0]
    return [(0, 0, n, a), (1, 0, n, forth), (3, 0, n, back), (2, 0, cut, far_a), (2, cut, n - cut, far_b)]


def swap_core(a):
    return lax.ppermute(a, "c", [(0, 1), (1, 0)])


def swap_half(a):
    return lax.ppermute(a, "zh", [(0, 1), (1, 0)])


def ring_z(a, by):
    return lax.ppermute(a, ("zh", "zl"), [(i, (i + by) % 8) for i in range(8)])


def head_slots(w, zl, y):
    parts = []
    for k in range(4):
        head = zl * 4 + (y + k) % 4
        one = lax.dynamic_slice_in_dim(w, head * 3 * HEAD_DIM, 3 * HEAD_DIM, axis=1)
        q, key, value = one[:, :HEAD_DIM], one[:, HEAD_DIM : 2 * HEAD_DIM], one[:, 2 * HEAD_DIM :]
        parts += [q, value[:, :FIRST], key, value[:, FIRST:], jnp.zeros((w.shape[0], 16), w.dtype)]
    return jnp.concatenate(parts, axis=1)


def shards(tokens, pre_gain, pre_shift, w_qkv, qkv_bias, w_out, out_bias, mlp_gain, mlp_shift, w_up, up_bias, w_down, down_bias):
    images, tok_here, width = tokens.shape
    row = lambda v: v.reshape(1, -1)
    x, zh, c, zl, y = (lax.axis_index(n) for n in ("x", "zh", "c", "zl", "y"))
    pos = jnp.stack([x, zh, c, zl, y]).astype(jnp.int32)

    gathered = []
    for i in range(images):
        own = tokens[i]
        ups, downs = [own], [own]
        for _ in range(3):
            ups.append(ring_z(ups[-1], 1))
            downs.append(ring_z(downs[-1], -1))
        gathered.append([own] + ups[1:] + downs[1:])

    slots = head_slots(w_qkv, zl, y)
    both = jnp.concatenate([slots, swap_half(slots)], axis=0)
    wq_pieces, wq_arrays = [], []
    for dx, row0, n, a in ring_gather(both, HEAD_DIM):
        for oc, b in ((0, a), (1, swap_core(a))):
            for oz in range(2):
                if row0 <= oz * HEAD_DIM < row0 + n:
                    wq_pieces.append((dx, oz, oc, 0, HEAD_DIM, oz * HEAD_DIM - row0))
                    wq_arrays.append(b)
    bias_slots = head_slots(row(qkv_bias), zl, y)
    ones = (jnp.arange(4 * SLOT) % SLOT == 240).astype(F32)
    bias_slots = bias_slots + row(ones)

    pack = jnp.concatenate([w_out, w_up[:, :width], w_up[:, width:], w_down], axis=0)
    padded = jnp.concatenate([pack, jnp.zeros((4 * QUARTER - pack.shape[0], width), BF)], axis=0)
    quarter = swap_half(lax.dynamic_slice_in_dim(padded, y * QUARTER, QUARTER, axis=0))
    quarters = jnp.concatenate([quarter] + [shift(quarter, "y", k, 4) for k in (1, 2, 3)], axis=0)
    own, own_arrays = [], []
    for dx, row0, n, a in ring_gather(pack, 208):
        for oc, b in ((0, a), (1, swap_core(a))):
            own.append((dx, 0, oc, row0, n, 0))
            own_arrays.append(b)
    other, other_arrays = [], []
    for dx, row0, n, a in ring_gather(quarters, 2 * QUARTER):
        for oc, b in ((0, a), (1, swap_core(a))):
            other.append((dx, 1, oc, row0 // QUARTER, n // QUARTER))
            other_arrays.append(b)

    packed = []
    for i in range(images):
        n_tok = len(gathered[i])
        packed.append(
            pl.pallas_call(
                lambda *refs, p=tuple(wq_pieces), n=n_tok: project_kernel(p, n, *refs),
                out_shape=jax.ShapeDtypeStruct((4, 4 * tok_here, SLOT), BF),
                in_specs=[SMEM] + [ANY] * (n_tok + len(wq_arrays)) + [VMEM] * 3,
                out_specs=VMEM,
                scratch_shapes=[
                    pltpu.VMEM((4 * tok_here, width), BF),
                    pltpu.VMEM((4 * tok_here, width), BF),
                    pltpu.VMEM((width, 4 * SLOT), BF),
                    pltpu.SemaphoreType.DMA((n_tok,)),
                    pltpu.SemaphoreType.DMA((len(wq_arrays),)),
                ],
                name=f"project{i}",
                cost_estimate=pl.CostEstimate(flops=2 * 576 * 1280 * 1024, bytes_accessed=6000000, transcendentals=0),
            )(pos, *gathered[i], *wq_arrays, row(pre_gain), row(pre_shift), bias_slots)
        )
    contexts = []
    for i in range(images):
        blocks = [packed[i][0]] + [shift(packed[i][k], "y", k, 4) for k in (1, 2, 3)]
        ctx = pl.pallas_call(
            lambda *refs: attend_kernel(288, *refs),
            out_shape=jax.ShapeDtypeStruct((HEADS, tok_here, LANES), BF),
            in_specs=[SMEM] + [ANY] * 4,
            out_specs=VMEM,
            scratch_shapes=[pltpu.VMEM((HEADS * tok_here, SLOT), BF), pltpu.SemaphoreType.DMA((4,))],
            name=f"attend{i}",
            cost_estimate=pl.CostEstimate(flops=4 * 2304 * 2304 * 256, bytes_accessed=2000000, transcendentals=2304 * 2304),
        )(pos, *blocks)
        contexts.append(lax.all_to_all(ctx, ("zl", "y"), split_axis=0, concat_axis=0, tiled=True))

    n_copies = len(own_arrays) + sum(o[4] for o in other)
    return pl.pallas_call(
        lambda *refs: finish_kernel(tuple(own), tuple(other), len(own_arrays), len(other_arrays), *refs),
        out_shape=jax.ShapeDtypeStruct(tokens.shape, BF),
        in_specs=[SMEM, VMEM, VMEM, VMEM] + [ANY] * (len(own_arrays) + len(other_arrays)) + [VMEM] * 5,
        out_specs=VMEM,
        scratch_shapes=[
            pltpu.VMEM((HEADS, 4 * QUARTER, width), BF),
            pltpu.VMEM((images * tok_here, width), F32),
            pltpu.VMEM((images * tok_here, width), BF),
            pltpu.VMEM((images * tok_here, 2 * width), BF),
            pltpu.SemaphoreType.DMA((n_copies,)),
        ],
        name="finish",
        cost_estimate=pl.CostEstimate(flops=4700000000, bytes_accessed=20000000, transcendentals=288 * 2560),
    )(pos, *contexts, tokens, *own_arrays, *other_arrays, row(out_bias), row(mlp_gain), row(mlp_shift), row(up_bias), row(down_bias))


def solution(mesh):
    dp, seq = ("x", "zh", "c"), ("zl", "y")
    fine = Mesh(mesh.devices.reshape(4, 2, 2, 4, 4), dp + seq)
    rows = P(dp, None)
    in_specs = (P(dp, seq, None), P(), P(), rows, P(), rows, P(), P(), P(), rows, P(), rows, P())
    return jax.shard_map(shards, mesh=fine, in_specs=in_specs, out_specs=P(dp, seq, None), check_vma=False)
```

```python
import math

import jax
import jax.numpy as jnp
from jax import lax
from jax.experimental import pallas as pl
from jax.experimental.pallas import tpu as pltpu
from jax.sharding import Mesh
from jax.sharding import PartitionSpec as P


HEADS = 16
HEAD_DIM = 80
EPSILON = 1e-05
LANES = 128
SLOT = 2 * LANES
FIRST = LANES - HEAD_DIM
QUARTER = 112
BF = jnp.bfloat16
F32 = jnp.float32
ANY = pl.BlockSpec(memory_space=pl.ANY)
SMEM = pl.BlockSpec(memory_space=pltpu.SMEM)
VMEM = pl.BlockSpec(memory_space=pltpu.VMEM)


def shift(a, axis, by, size):
    return lax.ppermute(a, axis, [(i, (i + by) % size) for i in range(size)])


def normalize(features, gain, shift_by):
    average = jnp.mean(features, axis=-1, keepdims=True)
    centered = features - average
    spread = jnp.mean(centered * centered, axis=-1, keepdims=True)
    return centered * lax.rsqrt(spread + EPSILON) * gain + shift_by


def run_copies(copies):
    for when, copy in copies:
        if when is None:
            copy.start()
        else:
            pl.when(when)(copy.start)


def wait_copies(copies):
    for when, copy in copies:
        if when is None:
            copy.wait()
        else:
            pl.when(when)(copy.wait)


def line(v, start=0, size=None):
    size = v.shape[0] if size is None else size
    return v[start : start + size].reshape(1, size)


def aligned(i, m):
    return pl.multiple_of(i * m, m)


def project_kernel(pieces, n_tok, pos, *refs):
    tok = refs[:n_tok]
    wts = refs[n_tok : n_tok + len(pieces)]
    gain, shift_by, bias, o0, o1, o2, o3, tok_s, nrm_s, w_s, sem_t, sem_w = refs[n_tok + len(pieces) :]
    x, zh, c, zl, y = pos[0], pos[1], pos[2], pos[3], pos[4]
    rows = tok[0].shape[0]
    moves = [(None, pltpu.make_async_copy(tok[0], tok_s.at[pl.ds(aligned(zl, rows), rows)], sem_t.at[0]))]
    for n in (1, 2, 3):
        up = pltpu.make_async_copy(tok[n], tok_s.at[pl.ds(aligned(jnp.maximum(zl - n, 0), rows), rows)], sem_t.at[n])
        down = pltpu.make_async_copy(tok[3 + n], tok_s.at[pl.ds(aligned(jnp.minimum(zl + n, 3), rows), rows)], sem_t.at[3 + n])
        moves.append((zl >= n, up))
        moves.append((zl + n <= 3, down))
    run_copies(moves)
    w_moves = []
    for i, (dx, oz, oc, row0, count, src0) in enumerate(pieces):
        d = ((x + 4 - dx) % 4) * 4 + ((zh + oz) % 2) * 2 + (c + oc) % 2
        dst = w_s.at[pl.ds(aligned(d, HEAD_DIM) + row0, count)]
        w_moves.append((None, pltpu.make_async_copy(wts[i].at[pl.ds(src0, count)], dst, sem_w.at[i])))
    run_copies(w_moves)
    wait_copies(moves)
    nrm_s[...] = normalize(tok_s[...].astype(F32), line(gain), line(shift_by)).astype(BF)
    wait_copies(w_moves)
    for k, out in enumerate((o0, o1, o2, o3)):
        cols = pl.ds(aligned((y + k) % 4, SLOT), SLOT)
        acc = jnp.dot(nrm_s[...], w_s[:, cols], preferred_element_type=F32)
        out[...] = (acc + bias[:, cols]).astype(BF)


def attend_kernel(block_rows, pos, b0, b1, b2, b3, out, s_ref, sem):
    y = pos[4]
    rows = b0.shape[0]
    part = rows // 4
    copies = [
        (None, pltpu.make_async_copy(b, s_ref.at[pl.ds(k * rows, rows)], sem.at[k]))
        for k, b in enumerate((b0, b1, b2, b3))
    ]
    run_copies(copies)
    wait_copies(copies)
    factor = math.log2(math.e) / math.sqrt(HEAD_DIM)
    lane = lax.broadcasted_iota(jnp.int32, (block_rows, LANES), 1)
    for r in range(4 * rows // block_rows):
        q = s_ref[r * block_rows : (r + 1) * block_rows, :LANES]
        q = jnp.where(lane < HEAD_DIM, q, jnp.zeros_like(q))
        scores = lax.dot_general(q, s_ref[:, LANES:], (((1,), (1,)), ((), ())), preferred_element_type=F32)
        highest = jnp.max(scores, axis=-1, keepdims=True)
        weights = jnp.exp2((scores - highest) * factor).astype(BF)
        mixed = jnp.dot(weights, s_ref[...], preferred_element_type=F32)
        total = mixed[:, 240:241]
        first = pltpu.roll(mixed[:, :LANES], LANES - HEAD_DIM, 1)
        second = pltpu.roll(mixed[:, LANES:], LANES - (HEAD_DIM - FIRST), 1)
        joined = jnp.where(lane < FIRST, first, second)
        joined = jnp.where(lane < HEAD_DIM, joined / total, 0.0).astype(BF)
        for p in range(block_rows // part):
            g = r * (block_rows // part) + p
            k, j = g // 4, g % 4
            out[j * 4 + (y + 4 - k) % 4] = joined[p * part : (p + 1) * part]


def finish_kernel(pos, c0, c1, tokens, gathered, out_bias, mlp_gain, mlp_shift, up_bias, down_bias, out, w_s, ctx_s, mid_s, nrm_s, hid_s, sem):
    zh = pos[1]
    moves = []
    for q in range(4):
        moves.append([])
        for xc in range(8):
            for oz in range(2):
                d = (xc // 2) * 4 + ((zh + oz) % 2) * 2 + xc % 2
                src = gathered.at[pl.ds(((xc * 4 + q) * 2 + oz) * QUARTER, QUARTER)]
                dst = w_s.at[d, pl.ds(q * QUARTER, QUARTER)]
                moves[q].append((None, pltpu.make_async_copy(src, dst, sem.at[(q * 8 + xc) * 2 + oz])))
    for group in moves:
        run_copies(group)
    rows, width = tokens.shape[1], tokens.shape[2]
    lane = lax.broadcasted_iota(jnp.int32, (rows, LANES), 1)
    for i, ctx in enumerate((c0, c1)):
        tiles = [None] * (width // LANES)
        for h in range(HEADS):
            t, off = divmod(h * HEAD_DIM, LANES)
            moved = ctx[h].astype(F32)
            if off:
                moved = pltpu.roll(moved, off, 1)
            if off == 0:
                tiles[t] = moved
                continue
            tiles[t] = jnp.where(lane >= off, moved, tiles[t])
            if off + HEAD_DIM > LANES:
                tiles[t + 1] = moved
        for t, tile in enumerate(tiles):
            ctx_s[i * rows : (i + 1) * rows, t * LANES : (t + 1) * LANES] = tile.astype(BF)
    wait_copies(moves[0])
    for n0 in range(0, width, SLOT):
        w = w_s[:, :HEAD_DIM, n0 : n0 + SLOT].reshape(width, SLOT)
        attended = jnp.dot(ctx_s[...], w, preferred_element_type=F32) + line(out_bias, n0, SLOT)
        for i in range(2):
            at = slice(i * rows, (i + 1) * rows)
            mid_s[at, n0 : n0 + SLOT] = tokens[i, :, n0 : n0 + SLOT].astype(F32) + attended[at]
    nrm_s[...] = normalize(mid_s[...], line(mlp_gain), line(mlp_shift)).astype(BF)
    wait_copies(moves[1])
    wait_copies(moves[2])
    for half in range(2):
        for n0 in range(0, width, SLOT):
            w = w_s[:, HEAD_DIM * (1 + half) : HEAD_DIM * (2 + half), n0 : n0 + SLOT].reshape(width, SLOT)
            at = half * width + n0
            lifted = jnp.dot(nrm_s[...], w, preferred_element_type=F32) + line(up_bias, at, SLOT)
            hid_s[:, at : at + SLOT] = (0.5 * lifted * (1.0 + lax.erf(lifted * math.sqrt(0.5)))).astype(BF)
    wait_copies(moves[3])
    for n0 in range(0, width, SLOT):
        w = w_s[:, HEAD_DIM * 3 : HEAD_DIM * 5, n0 : n0 + SLOT].reshape(2 * width, SLOT)
        lowered = jnp.dot(hid_s[...], w, preferred_element_type=F32)
        result = (mid_s[:, n0 : n0 + SLOT] + lowered + line(down_bias, n0, SLOT)).astype(BF)
        for i in range(2):
            out[i, :, n0 : n0 + SLOT] = result[i * rows : (i + 1) * rows]


def swap_core(a):
    return lax.ppermute(a, "c", [(0, 1), (1, 0)])


def swap_half(a):
    return lax.ppermute(a, "zh", [(0, 1), (1, 0)])


def ring_z(a, by):
    return lax.ppermute(a, ("zh", "zl"), [(i, (i + by) % 8) for i in range(8)])


def head_slots(w, zl):
    parts = []
    four = lax.dynamic_slice_in_dim(w, zl * 12 * HEAD_DIM, 12 * HEAD_DIM, axis=1)
    for k in range(4):
        one = four[:, k * 3 * HEAD_DIM : (k + 1) * 3 * HEAD_DIM]
        q, key, value = one[:, :HEAD_DIM], one[:, HEAD_DIM : 2 * HEAD_DIM], one[:, 2 * HEAD_DIM :]
        parts += [q, value[:, :FIRST], key, value[:, FIRST:], jnp.zeros((w.shape[0], 16), w.dtype)]
    return jnp.concatenate(parts, axis=1)


def shards(tokens, pre_gain, pre_shift, w_qkv, qkv_bias, w_out, out_bias, mlp_gain, mlp_shift, w_up, up_bias, w_down, down_bias):
    images, tok_here, width = tokens.shape
    row = lambda v: v.reshape(1, -1)
    x, zh, c, zl, y = (lax.axis_index(n) for n in ("x", "zh", "c", "zl", "y"))
    pos = jnp.stack([x, zh, c, zl, y]).astype(jnp.int32)

    gathered = []
    for i in range(images):
        own = tokens[i]
        ups, downs = [own], [own]
        for _ in range(3):
            ups.append(ring_z(ups[-1], 1))
            downs.append(ring_z(downs[-1], -1))
        gathered.append([own] + ups[1:] + downs[1:])

    slots = head_slots(w_qkv, zl)
    swapped = swap_half(slots)
    both = jnp.concatenate([slots, swapped], axis=0)
    wq_pieces, wq_arrays = [], []
    for dx in range(4):
        a = both if dx == 0 else shift(both, "x", dx, 4)
        across = swap_core(a)
        for oc, b in ((0, a), (1, across)):
            for oz in range(2):
                wq_pieces.append((dx, oz, oc, 0, HEAD_DIM, oz * HEAD_DIM))
                wq_arrays.append(b)
    bias_slots = head_slots(row(qkv_bias), zl)
    ones = (jnp.arange(4 * SLOT) % SLOT == 240).astype(F32)
    bias_slots = bias_slots + row(ones)

    pack = jnp.concatenate([w_out, w_up[:, :width], w_up[:, width:], w_down], axis=0)
    padded = jnp.concatenate([pack, jnp.zeros((4 * QUARTER - pack.shape[0], width), BF)], axis=0)
    quarter = lax.dynamic_slice_in_dim(padded, y * QUARTER, QUARTER, axis=0)
    swapped = swap_half(quarter)
    swapped = lax.optimization_barrier((swapped, gathered[0][2]))[0]
    quarters = jnp.concatenate([quarter, swapped], axis=0)
    weights = lax.all_gather(quarters, ("x", "c", "y"), axis=0, tiled=True)

    packed = []
    for i in range(images):
        n_tok = len(gathered[i])
        packed.append(
            pl.pallas_call(
                lambda *refs, p=tuple(wq_pieces), n=n_tok: project_kernel(p, n, *refs),
                out_shape=[jax.ShapeDtypeStruct((4 * tok_here, SLOT), BF)] * 4,
                in_specs=[SMEM] + [ANY] * (n_tok + len(wq_arrays)) + [VMEM] * 3,
                out_specs=[VMEM] * 4,
                scratch_shapes=[
                    pltpu.VMEM((4 * tok_here, width), BF),
                    pltpu.VMEM((4 * tok_here, width), BF),
                    pltpu.VMEM((width, 4 * SLOT), BF),
                    pltpu.SemaphoreType.DMA((n_tok,)),
                    pltpu.SemaphoreType.DMA((len(wq_arrays),)),
                ],
                cost_estimate=pl.CostEstimate(flops=2 * 576 * 1280 * 1024, bytes_accessed=6000000, transcendentals=0),
            )(pos, *gathered[i], *wq_arrays, pre_gain, pre_shift, bias_slots)
        )
    contexts = []
    for i in range(images):
        blocks = [packed[i][0]]
        for k in (1, 2, 3):
            blocks.append(shift(packed[i][k], "y", k, 4))
        call = pl.pallas_call(
            lambda *refs: attend_kernel(288, *refs),
            out_shape=jax.ShapeDtypeStruct((HEADS, tok_here, LANES), BF),
            in_specs=[SMEM] + [ANY] * 4,
            out_specs=VMEM,
            scratch_shapes=[pltpu.VMEM((HEADS * tok_here, SLOT), BF), pltpu.SemaphoreType.DMA((4,))],
            cost_estimate=pl.CostEstimate(flops=4 * 2304 * 2304 * 256, bytes_accessed=2000000, transcendentals=2304 * 2304),
        )
        ctx = call(pos, *blocks)
        contexts.append(lax.all_to_all(ctx, ("zl", "y"), split_axis=0, concat_axis=0, tiled=True))

    return pl.pallas_call(
        finish_kernel,
        out_shape=jax.ShapeDtypeStruct(tokens.shape, BF),
        in_specs=[SMEM, VMEM, VMEM, VMEM, ANY] + [VMEM] * 5,
        out_specs=VMEM,
        scratch_shapes=[
            pltpu.VMEM((HEADS, 4 * QUARTER, width), BF),
            pltpu.VMEM((images * tok_here, width), BF),
            pltpu.VMEM((images * tok_here, width), F32),
            pltpu.VMEM((images * tok_here, width), BF),
            pltpu.VMEM((images * tok_here, 2 * width), BF),
            pltpu.SemaphoreType.DMA((64,)),
        ],
        name="finish",
        cost_estimate=pl.CostEstimate(flops=4700000000, bytes_accessed=20000000, transcendentals=288 * 2560),
    )(pos, *contexts, tokens, weights, out_bias, mlp_gain, mlp_shift, up_bias, down_bias)


def solution(mesh):
    dp, seq = ("x", "zh", "c"), ("zl", "y")
    fine = Mesh(mesh.devices.reshape(4, 2, 2, 4, 4), dp + seq)
    rows = P(dp, None)
    in_specs = (P(dp, seq, None), P(), P(), rows, P(), rows, P(), P(), P(), rows, P(), rows, P())
    return jax.shard_map(shards, mesh=fine, in_specs=in_specs, out_specs=P(dp, seq, None), check_vma=False)
```

```python
import math

import jax
import jax.numpy as jnp
from jax import lax
from jax.experimental import pallas as pl
from jax.experimental.pallas import tpu as pltpu
from jax.sharding import Mesh
from jax.sharding import PartitionSpec as P


HEADS = 16
HEAD_DIM = 80
EPSILON = 1e-05
LANES = 128
SLOT = 2 * LANES
FIRST = LANES - HEAD_DIM
QUARTER = 112
USED = 112
BF = jnp.bfloat16
F32 = jnp.float32
ANY = pl.BlockSpec(memory_space=pltpu.HBM)
SMEM = pl.BlockSpec(memory_space=pltpu.SMEM)
VMEM = pl.BlockSpec(memory_space=pltpu.VMEM)


def shift(a, axis, by, size):
    return lax.ppermute(a, axis, [(i, (i + by) % size) for i in range(size)])


def normalize(features, gain, shift_by):
    average = jnp.mean(features, axis=-1, keepdims=True)
    centered = features - average
    spread = jnp.mean(centered * centered, axis=-1, keepdims=True)
    return centered * lax.rsqrt(spread + EPSILON) * gain + shift_by


def run_copies(copies):
    for when, copy in copies:
        if when is None:
            copy.start()
        else:
            pl.when(when)(copy.start)


def wait_copies(copies):
    for when, copy in copies:
        if when is None:
            copy.wait()
        else:
            pl.when(when)(copy.wait)


def line(v, start=0, size=None):
    size = v.shape[0] if size is None else size
    return v[start : start + size].reshape(1, size)


def aligned(i, m):
    return pl.multiple_of(i * m, m)


def prepare_kernel(pos, w_qkv, qkv_bias, w_out, w_up, w_down, slots, bias, pack, send, pad_s):
    zl, y = pos[3], pos[4]
    width = pack.shape[1]
    pad_s[: HEAD_DIM] = w_out[...]
    pad_s[HEAD_DIM : 2 * HEAD_DIM] = w_up[:, :width]
    pad_s[2 * HEAD_DIM : 3 * HEAD_DIM] = w_up[:, width:]
    pad_s[3 * HEAD_DIM : 5 * HEAD_DIM] = w_down[...]
    pad_s[5 * HEAD_DIM :] = jnp.zeros((4 * QUARTER - 5 * HEAD_DIM, width), BF)
    pack[...] = pad_s[: 5 * HEAD_DIM]
    send[HEAD_DIM:] = pad_s[pl.ds(aligned(y, QUARTER), QUARTER)]
    send[:HEAD_DIM, 4 * SLOT :] = jnp.zeros((HEAD_DIM, width - 4 * SLOT), BF)

    def two_tiles(window):
        lane = lax.broadcasted_iota(jnp.int32, (window.shape[0], LANES), 1)
        ahead = pltpu.roll(window, 3 * LANES - HEAD_DIM, 1)[:, :LANES]
        first = jnp.where(lane < HEAD_DIM, window[:, :LANES], ahead)
        second = jnp.where(lane < HEAD_DIM, ahead, window[:, LANES:SLOT])
        return first, second, lane

    def fill(group):
        for k in range(4):
            tile, off = divmod((4 * group + k) * 3 * HEAD_DIM, LANES)
            start = min(tile * LANES, w_qkv.shape[1] - 3 * LANES)
            off += tile * LANES - start
            turn = (3 * LANES - off) % (3 * LANES)
            w = w_qkv[:, start : start + 3 * LANES].astype(F32)
            v = jnp.broadcast_to(line(qkv_bias, start, 3 * LANES), (8, 3 * LANES))
            if turn:
                w, v = pltpu.roll(w, turn, 1), pltpu.roll(v, turn, 1)
            first, second, lane = two_tiles(w)
            both = jnp.concatenate([first, jnp.where(lane < USED, second, 0.0)], axis=1).astype(BF)
            slots[:, k * SLOT : (k + 1) * SLOT] = both
            send[:HEAD_DIM, k * SLOT : (k + 1) * SLOT] = both
            first, second, lane = two_tiles(v)
            second = jnp.where(lane < USED, second, jnp.where(lane == USED, 1.0, 0.0))
            bias[:, k * SLOT : (k + 1) * SLOT] = jnp.concatenate([first, second], axis=1)[:1]

    for group in range(4):
        pl.when(zl == group)(lambda group=group: fill(group))


def weight_copies(pieces, wts, w_s, sem, pos):
    x, zh, c = pos[0], pos[1], pos[2]
    moves = []
    for i, (dx, oz, oc) in enumerate(pieces):
        d = ((x + 4 - dx) % 4) * 4 + ((zh + oz) % 2) * 2 + (c + oc) % 2
        dst = w_s.at[pl.ds(aligned(d, HEAD_DIM), HEAD_DIM)]
        moves.append((None, pltpu.make_async_copy(wts[i].at[pl.ds(oz * HEAD_DIM, HEAD_DIM)], dst, sem.at[i])))
    return moves


def head_columns(pos, k):
    return pl.ds(aligned((pos[4] + k) % 4, SLOT), SLOT)


def project_kernel(pieces, pos, own, u1, u2, d1, d2, *refs):
    wts = refs[: len(pieces)]
    gain, shift_by, bias = refs[len(pieces) : len(pieces) + 3]
    outs = refs[len(pieces) + 3 : len(pieces) + 11]
    tok_s, nrm_s, w_s, sem_t, sem_w = refs[len(pieces) + 11 :]
    zl = pos[3]
    rows = own.shape[0]

    def copy_in(src, z, n):
        return pltpu.make_async_copy(src, tok_s.at[pl.ds(aligned(jnp.clip(z, 0, 3), rows), rows)], sem_t.at[n])

    moves = [
        (None, copy_in(own, zl, 0)),
        (zl >= 1, copy_in(u1, zl - 1, 1)),
        (zl >= 2, copy_in(u2, zl - 2, 2)),
        (zl <= 2, copy_in(d1, zl + 1, 3)),
        (zl <= 1, copy_in(d2, zl + 2, 4)),
        ((zl == 0) | (zl == 3), copy_in(own, 3 - zl, 5)),
    ]
    run_copies(moves)
    w_moves = weight_copies(pieces, wts, w_s, sem_w, pos)
    run_copies(w_moves)
    wait_copies(moves)
    nrm_s[...] = normalize(tok_s[...].astype(F32), line(gain), line(shift_by)).astype(BF)
    wait_copies(w_moves)
    part = rows // 2
    for k in range(4):
        cols = head_columns(pos, k)
        acc = jnp.dot(nrm_s[...], w_s[:, cols], preferred_element_type=F32)
        acc = (acc + bias[:, cols]).astype(BF)
        for z in range(4):
            for i in range(2):
                outs[i * 4 + k][z * part : (z + 1) * part] = acc[z * rows + i * part : z * rows + (i + 1) * part]


def late_kernel(pieces, pos, u3, d3, *refs):
    wts = refs[: len(pieces)]
    gain, shift_by, bias = refs[len(pieces) : len(pieces) + 3]
    outs = refs[len(pieces) + 11 : len(pieces) + 19]
    tok_s, nrm_s, w_s, out_s, sem_t, sem_w, sem_o = refs[len(pieces) + 19 :]
    zl = pos[3]
    rows = u3.shape[0]
    part = rows // 2

    @pl.when((zl == 0) | (zl == 3))
    def _():
        moves = [
            (zl == 3, pltpu.make_async_copy(u3, tok_s, sem_t.at[0])),
            (zl == 0, pltpu.make_async_copy(d3, tok_s, sem_t.at[1])),
        ]
        run_copies(moves)
        w_moves = weight_copies(pieces, wts, w_s, sem_w, pos)
        run_copies(w_moves)
        wait_copies(moves)
        nrm_s[...] = normalize(tok_s[...].astype(F32), line(gain), line(shift_by)).astype(BF)
        wait_copies(w_moves)
        out_moves = []
        for k in range(4):
            cols = head_columns(pos, k)
            acc = jnp.dot(nrm_s[...], w_s[:, cols], preferred_element_type=F32)
            out_s[k] = (acc + bias[:, cols]).astype(BF)
            for i in range(2):
                dst = outs[i * 4 + k].at[pl.ds(aligned(3 - zl, part), part)]
                copy = pltpu.make_async_copy(out_s.at[k, pl.ds(i * part, part)], dst, sem_o.at[i * 4 + k])
                out_moves.append((None, copy))
            run_copies(out_moves[-2:])
        wait_copies(out_moves)


def attend_kernel(block_rows, pos, b0, b1, b2, b3, out, s_ref, sem):
    y = pos[4]
    rows = b0.shape[0]
    part, third = rows // 4, rows // 12
    copies = [
        (None, pltpu.make_async_copy(b, s_ref.at[pl.ds(k * rows, rows)], sem.at[k]))
        for k, b in enumerate((b0, b1, b2, b3))
    ]
    run_copies(copies)
    wait_copies(copies)
    factor = math.log2(math.e) / math.sqrt(HEAD_DIM)
    lane = lax.broadcasted_iota(jnp.int32, (block_rows, LANES), 1)
    thin = lax.broadcasted_iota(jnp.int32, (third, LANES), 1)
    for r in range(4 * rows // block_rows):
        q = s_ref[r * block_rows : (r + 1) * block_rows, :LANES]
        q = jnp.where(lane < HEAD_DIM, q, jnp.zeros_like(q))
        scores = lax.dot_general(q, s_ref[:, LANES:], (((1,), (1,)), ((), ())), preferred_element_type=F32)
        highest = jnp.max(scores, axis=-1, keepdims=True)
        weights = jnp.exp2((scores - highest) * factor).astype(BF)
        mixed = jnp.dot(weights, s_ref[...], preferred_element_type=F32)
        total = mixed[:, LANES + USED : LANES + USED + 1]
        first = pltpu.roll(mixed[:, :LANES], LANES - HEAD_DIM, 1)
        second = pltpu.roll(mixed[:, LANES:], LANES - (HEAD_DIM - FIRST), 1)
        joined = jnp.where(lane < FIRST, first, second)
        joined = jnp.where(lane < HEAD_DIM, joined / total, 0.0)
        for p in range(block_rows // part):
            g = r * (block_rows // part) + p
            a, b, c = (joined[p * part + t * third : p * part + (t + 1) * third] for t in range(3))
            b, c = pltpu.roll(b, HEAD_DIM, 1), pltpu.roll(c, 2 * HEAD_DIM - LANES, 1)
            tile0 = jnp.where(thin < HEAD_DIM, a, b)
            tile1 = jnp.where(thin < 2 * HEAD_DIM - LANES, b, c)
            out[(g % 4) * 4 + (y + 4 - g // 4) % 4] = jnp.concatenate([tile0, tile1], axis=1).astype(BF)


def spread(block):
    lane = lax.broadcasted_iota(jnp.int32, (block.shape[0], LANES), 1)
    t0, t1 = block[:, :LANES].astype(F32), block[:, LANES:].astype(F32)
    back = LANES - HEAD_DIM
    middle = jnp.where(lane < back, pltpu.roll(t0, back, 1), pltpu.roll(t1, back, 1))
    parts = [t0, middle, pltpu.roll(t1, 2 * LANES - 2 * HEAD_DIM, 1)]
    return jnp.concatenate([jnp.where(lane < HEAD_DIM, p, 0.0) for p in parts], axis=0)


def finish_kernel(own, other, pos, c0, c1, tokens, *refs):
    own_w, other_w = refs[: len(own)], refs[len(own) : len(own) + len(other)]
    out_bias, mlp_gain, mlp_shift, up_bias, down_bias, out = refs[len(own) + len(other) :][:6]
    w_s, ctx_s, mid_s, nrm_s, hid_s, sem = refs[len(own) + len(other) + 6 :]
    x, zh, c, y = pos[0], pos[1], pos[2], pos[4]
    stages = [[], [], []]
    n = 0

    def place(dx, oz, oc):
        return ((x + 4 - dx) % 4) * 4 + ((zh + oz) % 2) * 2 + (c + oc) % 2

    for i, (dx, oc, row0, count) in enumerate(own):
        for stage, (low, high) in enumerate(((0, 1), (1, 3), (3, 5))):
            low, high = low * HEAD_DIM, high * HEAD_DIM
            if row0 <= low and high <= row0 + count:
                src = own_w[i].at[pl.ds(low - row0, high - low)]
                dst = w_s.at[place(dx, 0, oc), pl.ds(low, high - low)]
                stages[stage].append((None, pltpu.make_async_copy(src, dst, sem.at[n])))
                n += 1
    for i, (dx, oc, step0, steps) in enumerate(other):
        for q in range(4):
            k = (y + 4 - q) % 4
            inside = None if steps == 4 else (k >= step0) & (k < step0 + steps)
            at = jnp.clip(k - step0, 0, steps - 1)
            src = other_w[i].at[pl.ds(aligned(at, QUARTER), QUARTER)]
            dst = w_s.at[place(dx, 1, oc), pl.ds(q * QUARTER, QUARTER)]
            stages[(0, 1, 1, 2)[q]].append((inside, pltpu.make_async_copy(src, dst, sem.at[n])))
            n += 1
    for group in stages:
        run_copies(group)
    rows, width = tokens.shape[1], tokens.shape[2]
    lane = lax.broadcasted_iota(jnp.int32, (rows, LANES), 1)
    for i, ctx in enumerate((c0, c1)):
        tiles = [None] * (width // LANES)
        for h in range(HEADS):
            t, off = divmod(h * HEAD_DIM, LANES)
            moved = spread(ctx[h])
            if off == 0:
                tiles[t] = moved
                continue
            moved = pltpu.roll(moved, off, 1)
            tiles[t] = jnp.where(lane >= off, moved, tiles[t])
            if off + HEAD_DIM > LANES:
                tiles[t + 1] = moved
        for t, tile in enumerate(tiles):
            ctx_s[i * rows : (i + 1) * rows, t * LANES : (t + 1) * LANES] = tile.astype(BF)
    wait_copies(stages[0])
    for n0 in range(0, width, SLOT):
        w = w_s[:, :HEAD_DIM, n0 : n0 + SLOT].reshape(width, SLOT)
        attended = jnp.dot(ctx_s[...], w, preferred_element_type=F32) + line(out_bias, n0, SLOT)
        for i in range(2):
            at = slice(i * rows, (i + 1) * rows)
            mid_s[at, n0 : n0 + SLOT] = tokens[i, :, n0 : n0 + SLOT].astype(F32) + attended[at]
    nrm_s[...] = normalize(mid_s[...], line(mlp_gain), line(mlp_shift)).astype(BF)
    wait_copies(stages[1])
    for half in range(2):
        for n0 in range(0, width, SLOT):
            w = w_s[:, HEAD_DIM * (1 + half) : HEAD_DIM * (2 + half), n0 : n0 + SLOT].reshape(width, SLOT)
            at = half * width + n0
            lifted = jnp.dot(nrm_s[...], w, preferred_element_type=F32) + line(up_bias, at, SLOT)
            hid_s[:, at : at + SLOT] = (0.5 * lifted * (1.0 + lax.erf(lifted * math.sqrt(0.5)))).astype(BF)
    wait_copies(stages[2])
    for n0 in range(0, width, SLOT):
        w = w_s[:, HEAD_DIM * 3 : HEAD_DIM * 5, n0 : n0 + SLOT].reshape(2 * width, SLOT)
        lowered = jnp.dot(hid_s[...], w, preferred_element_type=F32)
        result = (mid_s[:, n0 : n0 + SLOT] + lowered + line(down_bias, n0, SLOT)).astype(BF)
        for i in range(2):
            out[i, :, n0 : n0 + SLOT] = result[i * rows : (i + 1) * rows]


def ring_gather(a):
    for dx in range(4):
        b = a if dx == 0 else shift(a, "x", dx, 4)
        across = swap_core(b)
        yield dx, 0, b
        yield dx, 1, across


def swap_core(a):
    return lax.ppermute(a, "c", [(0, 1), (1, 0)])


def swap_half(a):
    return lax.ppermute(a, "zh", [(0, 1), (1, 0)])


def ring_z(a, by):
    return lax.ppermute(a, ("zh", "zl"), [(i, (i + by) % 8) for i in range(8)])


def shards(tokens, pre_gain, pre_shift, w_qkv, qkv_bias, w_out, out_bias, mlp_gain, mlp_shift, w_up, up_bias, w_down, down_bias):
    images, tok_here, width = tokens.shape
    pos = jnp.stack([lax.axis_index(n) for n in ("x", "zh", "c", "zl", "y")]).astype(jnp.int32)

    ups, downs = [tokens.reshape(images * tok_here, width)], [tokens.reshape(images * tok_here, width)]
    for _ in range(3):
        ups.append(ring_z(ups[-1], 1))
        downs.append(ring_z(downs[-1], -1))

    slots, bias, pack, send = pl.pallas_call(
        prepare_kernel,
        out_shape=[
            jax.ShapeDtypeStruct((HEAD_DIM, 4 * SLOT), BF),
            jax.ShapeDtypeStruct((1, 4 * SLOT), F32),
            jax.ShapeDtypeStruct((5 * HEAD_DIM, width), BF),
            jax.ShapeDtypeStruct((HEAD_DIM + QUARTER, width), BF),
        ],
        in_specs=[SMEM] + [VMEM] * 5,
        out_specs=[VMEM] * 4,
        scratch_shapes=[pltpu.VMEM((4 * QUARTER, width), BF)],
        name="prepare",
    )(pos, w_qkv, qkv_bias, w_out, w_up, w_down)
    got = swap_half(send)

    both = jnp.concatenate([slots, got[:HEAD_DIM, : 4 * SLOT]], axis=0)
    wq_pieces, wq_arrays = [], []
    for dx in range(4):
        a = both if dx == 0 else shift(both, "x", dx, 4)
        across = swap_core(a)
        for oc, b in ((0, a), (1, across)):
            for oz in range(2):
                wq_pieces.append((dx, oz, oc))
                wq_arrays.append(b)

    quarters = [got[HEAD_DIM:]]
    for k in (1, 2, 3):
        quarters.append(shift(quarters[0], "y", k, 4))
    quarters = jnp.concatenate(quarters, axis=0)
    own, own_arrays, other, other_arrays = [], [], [], []
    for dx, oc, a in ring_gather(pack):
        own.append((dx, oc, 0, a.shape[0]))
        own_arrays.append(a)
    for dx, oc, a in ring_gather(quarters):
        other.append((dx, oc, 0, 4))
        other_arrays.append(a)

    rows = images * tok_here
    n_wq = len(wq_arrays)
    half = jax.ShapeDtypeStruct((4 * tok_here, SLOT), BF)
    project = pl.pallas_call(
        lambda *refs: project_kernel(tuple(wq_pieces), *refs),
        out_shape=[half] * 8,
        in_specs=[SMEM] + [ANY] * (5 + n_wq) + [VMEM] * 3,
        out_specs=[VMEM] * 8,
        scratch_shapes=[
            pltpu.VMEM((4 * rows, width), BF),
            pltpu.VMEM((4 * rows, width), BF),
            pltpu.VMEM((width, 4 * SLOT), BF),
            pltpu.SemaphoreType.DMA((6,)),
            pltpu.SemaphoreType.DMA((n_wq,)),
        ],
        name="project",
        cost_estimate=pl.CostEstimate(flops=2 * 1152 * 1280 * 1024, bytes_accessed=9000000, transcendentals=0),
    )
    late = pl.pallas_call(
        lambda *refs: late_kernel(tuple(wq_pieces), *refs),
        out_shape=[half] * 8,
        in_specs=[SMEM] + [ANY] * (2 + n_wq) + [VMEM] * 3 + [ANY] * 8,
        out_specs=[ANY] * 8,
        input_output_aliases={6 + n_wq + i: i for i in range(8)},
        scratch_shapes=[
            pltpu.VMEM((rows, width), BF),
            pltpu.VMEM((rows, width), BF),
            pltpu.VMEM((width, 4 * SLOT), BF),
            pltpu.VMEM((4, rows, SLOT), BF),
            pltpu.SemaphoreType.DMA((2,)),
            pltpu.SemaphoreType.DMA((n_wq,)),
            pltpu.SemaphoreType.DMA((8,)),
        ],
        name="late",
        cost_estimate=pl.CostEstimate(flops=2 * 288 * 1280 * 1024, bytes_accessed=4000000, transcendentals=0),
    )
    early = project(pos, ups[0], ups[1], ups[2], downs[1], downs[2], *wq_arrays, pre_gain, pre_shift, bias)
    packed = late(pos, ups[3], downs[3], *wq_arrays, pre_gain, pre_shift, bias, *early)

    contexts = []
    for i in range(images):
        attend = pl.pallas_call(
            lambda *refs: attend_kernel(288, *refs),
            out_shape=jax.ShapeDtypeStruct((HEADS, tok_here // 3, SLOT), BF),
            in_specs=[SMEM] + [ANY] * 4,
            out_specs=VMEM,
            scratch_shapes=[pltpu.VMEM((HEADS * tok_here, SLOT), BF), pltpu.SemaphoreType.DMA((4,))],
            cost_estimate=pl.CostEstimate(flops=4 * 2304 * 2304 * 256, bytes_accessed=2000000, transcendentals=2304 * 2304),
        )
        four = [packed[i * 4]]
        for k in (1, 2, 3):
            four.append(shift(packed[i * 4 + k], "y", k, 4))
        ctx = attend(pos, *four)
        contexts.append(lax.all_to_all(ctx, ("zl", "y"), split_axis=0, concat_axis=0, tiled=True))

    n_copies = 3 * len(own) + 4 * len(other)
    return pl.pallas_call(
        lambda *refs: finish_kernel(tuple(own), tuple(other), *refs),
        out_shape=jax.ShapeDtypeStruct(tokens.shape, BF),
        in_specs=[SMEM, VMEM, VMEM, VMEM] + [ANY] * (len(own) + len(other)) + [VMEM] * 5,
        out_specs=VMEM,
        scratch_shapes=[
            pltpu.VMEM((HEADS, 4 * QUARTER, width), BF),
            pltpu.VMEM((images * tok_here, width), BF),
            pltpu.VMEM((images * tok_here, width), F32),
            pltpu.VMEM((images * tok_here, width), BF),
            pltpu.VMEM((images * tok_here, 2 * width), BF),
            pltpu.SemaphoreType.DMA((n_copies,)),
        ],
        name="finish",
        cost_estimate=pl.CostEstimate(flops=4700000000, bytes_accessed=20000000, transcendentals=288 * 2560),
    )(pos, *contexts, tokens, *own_arrays, *other_arrays, out_bias, mlp_gain, mlp_shift, up_bias, down_bias)


def solution(mesh):
    dp, seq = ("x", "zh", "c"), ("zl", "y")
    fine = Mesh(mesh.devices.reshape(4, 2, 2, 4, 4), dp + seq)
    rows = P(dp, None)
    in_specs = (P(dp, seq, None), P(), P(), rows, P(), rows, P(), P(), P(), rows, P(), rows, P())
    return jax.shard_map(shards, mesh=fine, in_specs=in_specs, out_specs=P(dp, seq, None), check_vma=False)
```

```python
import math

import jax
import jax.numpy as jnp
from jax import lax
from jax.experimental import pallas as pl
from jax.experimental.pallas import tpu as pltpu
from jax.sharding import Mesh
from jax.sharding import PartitionSpec as P


HEADS = 16
HEAD_DIM = 80
EPSILON = 1e-05
LANES = 128
SLOT = 2 * LANES
FIRST = LANES - HEAD_DIM
QUARTER = 112
USED = 112
BF = jnp.bfloat16
F32 = jnp.float32
ANY = pl.BlockSpec(memory_space=pltpu.HBM)
SMEM = pl.BlockSpec(memory_space=pltpu.SMEM)
VMEM = pl.BlockSpec(memory_space=pltpu.VMEM)


def shift(a, axis, by, size):
    return lax.ppermute(a, axis, [(i, (i + by) % size) for i in range(size)])


def normalize(features, gain, shift_by):
    average = jnp.mean(features, axis=-1, keepdims=True)
    centered = features - average
    spread = jnp.mean(centered * centered, axis=-1, keepdims=True)
    return centered * lax.rsqrt(spread + EPSILON) * gain + shift_by


def normalize_rows(src, dst, gain, shift_by, step):
    def some(n, carry):
        at = pl.ds(aligned(n, step), step)
        dst[at] = normalize(src[at].astype(F32), line(gain), line(shift_by)).astype(BF)
        return carry

    lax.fori_loop(0, src.shape[0] // step, some, 0)


def join_kernel(*refs):
    parts, out, sem = refs[:-2], refs[-2], refs[-1]
    rows = parts[0].shape[0]
    copies = [(None, pltpu.make_async_copy(p, out.at[pl.ds(i * rows, rows)], sem.at[i])) for i, p in enumerate(parts)]
    run_copies(copies)
    wait_copies(copies)


def join(parts):
    rows, width = parts[0].shape
    return pl.pallas_call(
        join_kernel,
        out_shape=jax.ShapeDtypeStruct((len(parts) * rows, width), BF),
        in_specs=[ANY] * len(parts),
        out_specs=ANY,
        scratch_shapes=[pltpu.SemaphoreType.DMA((len(parts),))],
        name="join",
    )(*parts)


def run_copies(copies):
    for when, copy in copies:
        if when is None:
            copy.start()
        else:
            pl.when(when)(copy.start)


def wait_copies(copies):
    for when, copy in copies:
        if when is None:
            copy.wait()
        else:
            pl.when(when)(copy.wait)


def line(v, start=0, size=None):
    size = v.shape[0] if size is None else size
    return v[start : start + size].reshape(1, size)


def aligned(i, m):
    return pl.multiple_of(i * m, m)


def prepare_kernel(pos, w_qkv, qkv_bias, w_out, w_up, w_down, slots, bias, pack, quarter, pad_s):
    zl, y = pos[3], pos[4]
    width = pack.shape[1]
    pad_s[: HEAD_DIM] = w_out[...]
    pad_s[HEAD_DIM : 2 * HEAD_DIM] = w_up[:, :width]
    pad_s[2 * HEAD_DIM : 3 * HEAD_DIM] = w_up[:, width:]
    pad_s[3 * HEAD_DIM : 5 * HEAD_DIM] = w_down[...]
    pad_s[5 * HEAD_DIM :] = jnp.zeros((4 * QUARTER - 5 * HEAD_DIM, width), BF)
    pack[...] = pad_s[: 5 * HEAD_DIM]
    quarter[...] = pad_s[pl.ds(aligned(y, QUARTER), QUARTER)]

    def two_tiles(window):
        lane = lax.broadcasted_iota(jnp.int32, (window.shape[0], LANES), 1)
        ahead = pltpu.roll(window, 3 * LANES - HEAD_DIM, 1)[:, :LANES]
        first = jnp.where(lane < HEAD_DIM, window[:, :LANES], ahead)
        second = jnp.where(lane < HEAD_DIM, ahead, window[:, LANES:SLOT])
        return first, second, lane

    for k in range(4):
        first_column = (4 * zl + k) * 3 * HEAD_DIM
        start = jnp.minimum(first_column // LANES, w_qkv.shape[1] // LANES - 3)
        turn = (3 * LANES - (first_column - start * LANES)) % (3 * LANES)
        cols = pl.ds(aligned(start, LANES), 3 * LANES)
        w = pltpu.roll(w_qkv[:, cols].astype(F32), turn, 1)
        v = pltpu.roll(jnp.broadcast_to(qkv_bias[:, cols], (8, 3 * LANES)), turn, 1)
        first, second, lane = two_tiles(w)
        both = jnp.concatenate([first, jnp.where(lane < USED, second, 0.0)], axis=1)
        slots[:, k * SLOT : (k + 1) * SLOT] = both.astype(BF)
        first, second, lane = two_tiles(v)
        second = jnp.where(lane < USED, second, jnp.where(lane == USED, 1.0, 0.0))
        bias[:, k * SLOT : (k + 1) * SLOT] = jnp.concatenate([first, second], axis=1)[:1]


def weight_copies(pieces, wts, w_s, sem, pos):
    x, zh, c = pos[0], pos[1], pos[2]
    moves = []
    for i, (dx, oz, oc) in enumerate(pieces):
        d = ((x + 4 - dx) % 4) * 4 + ((zh + oz) % 2) * 2 + (c + oc) % 2
        dst = w_s.at[pl.ds(aligned(d, HEAD_DIM), HEAD_DIM)]
        moves.append((None, pltpu.make_async_copy(wts[i].at[pl.ds(oz * HEAD_DIM, HEAD_DIM)], dst, sem.at[i])))
    return moves


def head_columns(pos, k):
    return pl.ds(aligned((pos[4] + k) % 4, SLOT), SLOT)


def project_kernel(pieces, pos, own, u1, u2, d1, d2, *refs):
    wts = refs[: len(pieces)]
    gain, shift_by, bias = refs[len(pieces) : len(pieces) + 3]
    outs = refs[len(pieces) + 3 : len(pieces) + 11]
    tok_s, nrm_s, w_s, sem_t, sem_w = refs[len(pieces) + 11 :]
    zl = pos[3]
    rows = own.shape[0]

    def copy_in(src, z, n):
        return pltpu.make_async_copy(src, tok_s.at[pl.ds(aligned(jnp.clip(z, 0, 3), rows), rows)], sem_t.at[n])

    moves = [
        (None, copy_in(own, zl, 0)),
        (zl >= 1, copy_in(u1, zl - 1, 1)),
        (zl >= 2, copy_in(u2, zl - 2, 2)),
        (zl <= 2, copy_in(d1, zl + 1, 3)),
        (zl <= 1, copy_in(d2, zl + 2, 4)),
        ((zl == 0) | (zl == 3), copy_in(own, 3 - zl, 5)),
    ]
    run_copies(moves)
    w_moves = weight_copies(pieces, wts, w_s, sem_w, pos)
    run_copies(w_moves)
    wait_copies(moves)
    normalize_rows(tok_s, nrm_s, gain, shift_by, 96)
    wait_copies(w_moves)
    part = rows // 2
    for k in range(4):
        cols = head_columns(pos, k)
        acc = jnp.dot(nrm_s[...], w_s[:, cols], preferred_element_type=F32)
        acc = (acc + bias[:, cols]).astype(BF)
        for z in range(4):
            for i in range(2):
                outs[i * 4 + k][z * part : (z + 1) * part] = acc[z * rows + i * part : z * rows + (i + 1) * part]


def late_kernel(pieces, pos, u3, d3, *refs):
    wts = refs[: len(pieces)]
    gain, shift_by, bias = refs[len(pieces) : len(pieces) + 3]
    outs = refs[len(pieces) + 11 : len(pieces) + 19]
    tok_s, nrm_s, w_s, out_s, sem_t, sem_w, sem_o = refs[len(pieces) + 19 :]
    zl = pos[3]
    rows = u3.shape[0]
    part = rows // 2

    @pl.when((zl == 0) | (zl == 3))
    def _():
        moves = [
            (zl == 3, pltpu.make_async_copy(u3, tok_s, sem_t.at[0])),
            (zl == 0, pltpu.make_async_copy(d3, tok_s, sem_t.at[1])),
        ]
        run_copies(moves)
        w_moves = weight_copies(pieces, wts, w_s, sem_w, pos)
        run_copies(w_moves)
        wait_copies(moves)
        normalize_rows(tok_s, nrm_s, gain, shift_by, 96)
        wait_copies(w_moves)
        out_moves = []
        for k in range(4):
            cols = head_columns(pos, k)
            acc = jnp.dot(nrm_s[...], w_s[:, cols], preferred_element_type=F32)
            out_s[k] = (acc + bias[:, cols]).astype(BF)
            for i in range(2):
                dst = outs[i * 4 + k].at[pl.ds(aligned(3 - zl, part), part)]
                copy = pltpu.make_async_copy(out_s.at[k, pl.ds(i * part, part)], dst, sem_o.at[i * 4 + k])
                out_moves.append((None, copy))
            run_copies(out_moves[-2:])
        wait_copies(out_moves)


def attend_kernel(block_rows, pos, b0, b1, b2, b3, out, s_ref, sem):
    y = pos[4]
    rows = b0.shape[0]
    part, third = rows // 4, rows // 12
    copies = [
        (None, pltpu.make_async_copy(b, s_ref.at[pl.ds(k * rows, rows)], sem.at[k]))
        for k, b in enumerate((b0, b1, b2, b3))
    ]
    run_copies(copies)
    wait_copies(copies)
    factor = math.log2(math.e) / math.sqrt(HEAD_DIM)
    lane = lax.broadcasted_iota(jnp.int32, (block_rows, LANES), 1)
    thin = lax.broadcasted_iota(jnp.int32, (third, LANES), 1)

    def one(r, carry):
        at = pl.ds(aligned(r, block_rows), block_rows)
        q = s_ref[at, :LANES]
        q = jnp.where(lane < HEAD_DIM, q, jnp.zeros_like(q))
        scores = lax.dot_general(q, s_ref[:, LANES:], (((1,), (1,)), ((), ())), preferred_element_type=F32)
        highest = jnp.max(scores, axis=-1, keepdims=True)
        weights = jnp.exp2((scores - highest) * factor).astype(BF)
        mixed = jnp.dot(weights, s_ref[...], preferred_element_type=F32)
        total = mixed[:, LANES + USED : LANES + USED + 1]
        first = pltpu.roll(mixed[:, :LANES], LANES - HEAD_DIM, 1)
        second = pltpu.roll(mixed[:, LANES:], LANES - (HEAD_DIM - FIRST), 1)
        joined = jnp.where(lane < FIRST, first, second)
        joined = jnp.where(lane < HEAD_DIM, joined / total, 0.0)
        for p in range(block_rows // part):
            g = r * (block_rows // part) + p
            a, b, c = (joined[p * part + t * third : p * part + (t + 1) * third] for t in range(3))
            b, c = pltpu.roll(b, HEAD_DIM, 1), pltpu.roll(c, 2 * HEAD_DIM - LANES, 1)
            tile0 = jnp.where(thin < HEAD_DIM, a, b)
            tile1 = jnp.where(thin < 2 * HEAD_DIM - LANES, b, c)
            out[(g % 4) * 4 + (y + 4 - g // 4) % 4] = jnp.concatenate([tile0, tile1], axis=1).astype(BF)
        return carry

    lax.fori_loop(0, 4 * rows // block_rows, one, 0)


def spread(block):
    lane = lax.broadcasted_iota(jnp.int32, (block.shape[0], LANES), 1)
    t0, t1 = block[:, :LANES].astype(F32), block[:, LANES:].astype(F32)
    back = LANES - HEAD_DIM
    middle = jnp.where(lane < back, pltpu.roll(t0, back, 1), pltpu.roll(t1, back, 1))
    parts = [t0, middle, pltpu.roll(t1, 2 * LANES - 2 * HEAD_DIM, 1)]
    return jnp.concatenate([jnp.where(lane < HEAD_DIM, p, 0.0) for p in parts], axis=0)


def finish_kernel(own, other, pos, c0, c1, tokens, *refs):
    own_w, other_w = refs[: len(own)], refs[len(own) : len(own) + len(other)]
    out_bias, mlp_gain, mlp_shift, up_bias, down_bias, out = refs[len(own) + len(other) :][:6]
    w_s, ctx_s, mid_s, nrm_s, hid_s, sem = refs[len(own) + len(other) + 6 :]
    x, zh, c, y = pos[0], pos[1], pos[2], pos[4]
    stages = [[], [], []]
    n = 0

    def place(dx, oz, oc):
        return ((x + 4 - dx) % 4) * 4 + ((zh + oz) % 2) * 2 + (c + oc) % 2

    for i, (dx, oc, row0, count) in enumerate(own):
        for stage, (low, high) in enumerate(((0, 1), (1, 3), (3, 5))):
            low, high = low * HEAD_DIM, high * HEAD_DIM
            if row0 <= low and high <= row0 + count:
                src = own_w[i].at[pl.ds(low - row0, high - low)]
                dst = w_s.at[place(dx, 0, oc), pl.ds(low, high - low)]
                stages[stage].append((None, pltpu.make_async_copy(src, dst, sem.at[n])))
                n += 1
    for i, (dx, oc, step0, steps) in enumerate(other):
        for q in range(4):
            k = (y + 4 - q) % 4
            inside = None if steps == 4 else (k >= step0) & (k < step0 + steps)
            at = jnp.clip(k - step0, 0, steps - 1)
            src = other_w[i].at[pl.ds(aligned(at, QUARTER), QUARTER)]
            dst = w_s.at[place(dx, 1, oc), pl.ds(q * QUARTER, QUARTER)]
            stages[(0, 1, 1, 2)[q]].append((inside, pltpu.make_async_copy(src, dst, sem.at[n])))
            n += 1
    for group in stages:
        run_copies(group)
    rows, width = tokens.shape[1], tokens.shape[2]
    lane = lax.broadcasted_iota(jnp.int32, (rows, LANES), 1)
    for i, ctx in enumerate((c0, c1)):
        tiles = [None] * (width // LANES)
        for h in range(HEADS):
            t, off = divmod(h * HEAD_DIM, LANES)
            moved = spread(ctx[h])
            if off == 0:
                tiles[t] = moved
                continue
            moved = pltpu.roll(moved, off, 1)
            tiles[t] = jnp.where(lane >= off, moved, tiles[t])
            if off + HEAD_DIM > LANES:
                tiles[t + 1] = moved
        for t, tile in enumerate(tiles):
            ctx_s[i * rows : (i + 1) * rows, t * LANES : (t + 1) * LANES] = tile.astype(BF)
    wait_copies(stages[0])

    def project_out(n, carry):
        cols = pl.ds(aligned(n, SLOT), SLOT)
        w = w_s[:, :HEAD_DIM, cols].reshape(width, SLOT)
        attended = jnp.dot(ctx_s[...], w, preferred_element_type=F32) + out_bias[cols].reshape(1, SLOT)
        for i in range(2):
            at = slice(i * rows, (i + 1) * rows)
            mid_s[at, cols] = tokens[i, :, cols].astype(F32) + attended[at]
        return carry

    lax.fori_loop(0, width // SLOT, project_out, 0)
    normalize_rows(mid_s, nrm_s, mlp_gain, mlp_shift, 96)
    wait_copies(stages[1])

    def lift(n, carry):
        for half in range(2):
            cols = pl.ds(aligned(n, SLOT), SLOT)
            to = pl.ds(aligned(n + half * (width // SLOT), SLOT), SLOT)
            w = w_s[:, HEAD_DIM * (1 + half) : HEAD_DIM * (2 + half), cols].reshape(width, SLOT)
            lifted = jnp.dot(nrm_s[...], w, preferred_element_type=F32) + up_bias[to].reshape(1, SLOT)
            hid_s[:, to] = (0.5 * lifted * (1.0 + lax.erf(lifted * math.sqrt(0.5)))).astype(BF)
        return carry

    lax.fori_loop(0, width // SLOT, lift, 0)
    wait_copies(stages[2])

    def lower(n, carry):
        cols = pl.ds(aligned(n, SLOT), SLOT)
        w = w_s[:, HEAD_DIM * 3 : HEAD_DIM * 5, cols].reshape(2 * width, SLOT)
        lowered = jnp.dot(hid_s[...], w, preferred_element_type=F32)
        result = (mid_s[:, cols] + lowered + down_bias[cols].reshape(1, SLOT)).astype(BF)
        for i in range(2):
            out[i, :, cols] = result[i * rows : (i + 1) * rows]
        return carry

    lax.fori_loop(0, width // SLOT, lower, 0)


def ring_gather(a):
    for dx in range(4):
        b = a if dx == 0 else shift(a, "x", dx, 4)
        across = swap_core(b)
        yield dx, 0, b
        yield dx, 1, across


def swap_core(a):
    return lax.ppermute(a, "c", [(0, 1), (1, 0)])


def swap_half(a):
    return lax.ppermute(a, "zh", [(0, 1), (1, 0)])


def ring_z(a, by):
    return lax.ppermute(a, ("zh", "zl"), [(i, (i + by) % 8) for i in range(8)])


def shards(tokens, pre_gain, pre_shift, w_qkv, qkv_bias, w_out, out_bias, mlp_gain, mlp_shift, w_up, up_bias, w_down, down_bias):
    images, tok_here, width = tokens.shape
    pos = jnp.stack([lax.axis_index(n) for n in ("x", "zh", "c", "zl", "y")]).astype(jnp.int32)

    ups, downs = [tokens.reshape(images * tok_here, width)], [tokens.reshape(images * tok_here, width)]
    for _ in range(3):
        ups.append(ring_z(ups[-1], 1))
        downs.append(ring_z(downs[-1], -1))

    slots, bias, pack, quarter = pl.pallas_call(
        prepare_kernel,
        out_shape=[
            jax.ShapeDtypeStruct((HEAD_DIM, 4 * SLOT), BF),
            jax.ShapeDtypeStruct((1, 4 * SLOT), F32),
            jax.ShapeDtypeStruct((5 * HEAD_DIM, width), BF),
            jax.ShapeDtypeStruct((QUARTER, width), BF),
        ],
        in_specs=[SMEM] + [VMEM] * 5,
        out_specs=[VMEM] * 4,
        scratch_shapes=[pltpu.VMEM((4 * QUARTER, width), BF)],
        name="prepare",
    )(pos, w_qkv, qkv_bias.reshape(1, -1), w_out, w_up, w_down)
    got = swap_half(slots)
    quarters = [swap_half(quarter)]

    both = join([slots, got])
    wq_pieces, wq_arrays = [], []
    for dx in range(4):
        a = both if dx == 0 else shift(both, "x", dx, 4)
        across = swap_core(a)
        for oc, b in ((0, a), (1, across)):
            for oz in range(2):
                wq_pieces.append((dx, oz, oc))
                wq_arrays.append(b)

    for k in (1, 2, 3):
        quarters.append(shift(quarters[0], "y", k, 4))
    quarters = join(quarters)
    own, own_arrays, other, other_arrays = [], [], [], []
    for dx, oc, a in ring_gather(pack):
        own.append((dx, oc, 0, a.shape[0]))
        own_arrays.append(a)
    for dx, oc, a in ring_gather(quarters):
        other.append((dx, oc, 0, 4))
        other_arrays.append(a)

    rows = images * tok_here
    n_wq = len(wq_arrays)
    half = jax.ShapeDtypeStruct((4 * tok_here, SLOT), BF)
    project = pl.pallas_call(
        lambda *refs: project_kernel(tuple(wq_pieces), *refs),
        out_shape=[half] * 8,
        in_specs=[SMEM] + [ANY] * (5 + n_wq) + [VMEM] * 3,
        out_specs=[VMEM] * 8,
        scratch_shapes=[
            pltpu.VMEM((4 * rows, width), BF),
            pltpu.VMEM((4 * rows, width), BF),
            pltpu.VMEM((width, 4 * SLOT), BF),
            pltpu.SemaphoreType.DMA((6,)),
            pltpu.SemaphoreType.DMA((n_wq,)),
        ],
        name="project",
        cost_estimate=pl.CostEstimate(flops=2 * 1152 * 1280 * 1024, bytes_accessed=9000000, transcendentals=0),
    )
    late = pl.pallas_call(
        lambda *refs: late_kernel(tuple(wq_pieces), *refs),
        out_shape=[half] * 8,
        in_specs=[SMEM] + [ANY] * (2 + n_wq) + [VMEM] * 3 + [ANY] * 8,
        out_specs=[ANY] * 8,
        input_output_aliases={6 + n_wq + i: i for i in range(8)},
        scratch_shapes=[
            pltpu.VMEM((rows, width), BF),
            pltpu.VMEM((rows, width), BF),
            pltpu.VMEM((width, 4 * SLOT), BF),
            pltpu.VMEM((4, rows, SLOT), BF),
            pltpu.SemaphoreType.DMA((2,)),
            pltpu.SemaphoreType.DMA((n_wq,)),
            pltpu.SemaphoreType.DMA((8,)),
        ],
        name="late",
        cost_estimate=pl.CostEstimate(flops=2 * 288 * 1280 * 1024, bytes_accessed=4000000, transcendentals=0),
    )
    early = project(pos, ups[0], ups[1], ups[2], downs[1], downs[2], *wq_arrays, pre_gain, pre_shift, bias)
    packed = late(pos, ups[3], downs[3], *wq_arrays, pre_gain, pre_shift, bias, *early)

    contexts = []
    for i in range(images):
        attend = pl.pallas_call(
            lambda *refs: attend_kernel(288, *refs),
            out_shape=jax.ShapeDtypeStruct((HEADS, tok_here // 3, SLOT), BF),
            in_specs=[SMEM] + [ANY] * 4,
            out_specs=VMEM,
            scratch_shapes=[pltpu.VMEM((HEADS * tok_here, SLOT), BF), pltpu.SemaphoreType.DMA((4,))],
            cost_estimate=pl.CostEstimate(flops=4 * 2304 * 2304 * 256, bytes_accessed=2000000, transcendentals=2304 * 2304),
        )
        four = [packed[i * 4]]
        for k in (1, 2, 3):
            four.append(shift(packed[i * 4 + k], "y", k, 4))
        ctx = attend(pos, *four)
        contexts.append(lax.all_to_all(ctx, ("zl", "y"), split_axis=0, concat_axis=0, tiled=True))

    n_copies = 3 * len(own) + 4 * len(other)
    return pl.pallas_call(
        lambda *refs: finish_kernel(tuple(own), tuple(other), *refs),
        out_shape=jax.ShapeDtypeStruct(tokens.shape, BF),
        in_specs=[SMEM, VMEM, VMEM, VMEM] + [ANY] * (len(own) + len(other)) + [VMEM] * 5,
        out_specs=VMEM,
        scratch_shapes=[
            pltpu.VMEM((HEADS, 4 * QUARTER, width), BF),
            pltpu.VMEM((images * tok_here, width), BF),
            pltpu.VMEM((images * tok_here, width), F32),
            pltpu.VMEM((images * tok_here, width), BF),
            pltpu.VMEM((images * tok_here, 2 * width), BF),
            pltpu.SemaphoreType.DMA((n_copies,)),
        ],
        name="finish",
        cost_estimate=pl.CostEstimate(flops=4700000000, bytes_accessed=20000000, transcendentals=288 * 2560),
    )(pos, *contexts, tokens, *own_arrays, *other_arrays, out_bias, mlp_gain, mlp_shift, up_bias, down_bias)


def solution(mesh):
    dp, seq = ("x", "zh", "c"), ("zl", "y")
    fine = Mesh(mesh.devices.reshape(4, 2, 2, 4, 4), dp + seq)
    rows = P(dp, None)
    in_specs = (P(dp, seq, None), P(), P(), rows, P(), rows, P(), P(), P(), rows, P(), rows, P())
    return jax.shard_map(shards, mesh=fine, in_specs=in_specs, out_specs=P(dp, seq, None), check_vma=False)
```

```python
import math

import jax
import jax.numpy as jnp
from jax import lax
from jax.experimental import pallas as pl
from jax.experimental.pallas import tpu as pltpu
from jax.sharding import Mesh
from jax.sharding import PartitionSpec as P


HEADS = 16
HEAD_DIM = 80
EPSILON = 1e-05
LANES = 128
SLOT = 2 * LANES
FIRST = LANES - HEAD_DIM
QUARTER = 112
USED = 112
BF = jnp.bfloat16
F32 = jnp.float32
ANY = pl.BlockSpec(memory_space=pltpu.HBM)
SMEM = pl.BlockSpec(memory_space=pltpu.SMEM)
VMEM = pl.BlockSpec(memory_space=pltpu.VMEM)


def shift(a, axis, by, size):
    return lax.ppermute(a, axis, [(i, (i + by) % size) for i in range(size)])


def normalize(features, gain, shift_by):
    average = jnp.mean(features, axis=-1, keepdims=True)
    centered = features - average
    spread = jnp.mean(centered * centered, axis=-1, keepdims=True)
    return centered * lax.rsqrt(spread + EPSILON) * gain + shift_by


def normalize_rows(src, dst, gain, shift_by, step):
    def some(n, carry):
        at = pl.ds(aligned(n, step), step)
        dst[at] = normalize(src[at].astype(F32), line(gain), line(shift_by)).astype(BF)
        return carry

    lax.fori_loop(0, src.shape[0] // step, some, 0)


def join_kernel(*refs):
    parts, out = refs[:-1], refs[-1]
    rows = parts[0].shape[0]
    for i, part in enumerate(parts):
        out[i * rows : (i + 1) * rows] = part[...]


def run_copies(copies):
    for when, copy in copies:
        if when is None:
            copy.start()
        else:
            pl.when(when)(copy.start)


def wait_copies(copies):
    for when, copy in copies:
        if when is None:
            copy.wait()
        else:
            pl.when(when)(copy.wait)


def line(v, start=0, size=None):
    size = v.shape[0] if size is None else size
    return v[start : start + size].reshape(1, size)


def aligned(i, m):
    return pl.multiple_of(i * m, m)


def prepare_kernel(pos, w_qkv, qkv_bias, w_out, w_up, w_down, slots, bias, pack, quarter, pad_s):
    zl, y = pos[3], pos[4]
    width = pack.shape[1]
    pad_s[: HEAD_DIM] = w_out[...]
    pad_s[HEAD_DIM : 2 * HEAD_DIM] = w_up[:, :width]
    pad_s[2 * HEAD_DIM : 3 * HEAD_DIM] = w_up[:, width:]
    pad_s[3 * HEAD_DIM : 5 * HEAD_DIM] = w_down[...]
    pad_s[5 * HEAD_DIM :] = jnp.zeros((4 * QUARTER - 5 * HEAD_DIM, width), BF)
    pack[...] = pad_s[: 5 * HEAD_DIM]
    quarter[...] = pad_s[pl.ds(aligned(y, QUARTER), QUARTER)]

    def two_tiles(window):
        lane = lax.broadcasted_iota(jnp.int32, (window.shape[0], LANES), 1)
        ahead = pltpu.roll(window, 3 * LANES - HEAD_DIM, 1)[:, :LANES]
        first = jnp.where(lane < HEAD_DIM, window[:, :LANES], ahead)
        second = jnp.where(lane < HEAD_DIM, ahead, window[:, LANES:SLOT])
        return first, second, lane

    for k in range(4):
        first_column = (4 * zl + k) * 3 * HEAD_DIM
        start = jnp.minimum(first_column // LANES, w_qkv.shape[1] // LANES - 3)
        turn = (3 * LANES - (first_column - start * LANES)) % (3 * LANES)
        cols = pl.ds(aligned(start, LANES), 3 * LANES)
        w = pltpu.roll(w_qkv[:, cols].astype(F32), turn, 1)
        v = pltpu.roll(jnp.broadcast_to(qkv_bias[:, cols], (8, 3 * LANES)), turn, 1)
        first, second, lane = two_tiles(w)
        both = jnp.concatenate([first, jnp.where(lane < USED, second, 0.0)], axis=1)
        slots[:, k * SLOT : (k + 1) * SLOT] = both.astype(BF)
        first, second, lane = two_tiles(v)
        second = jnp.where(lane < USED, second, jnp.where(lane == USED, 1.0, 0.0))
        bias[:, k * SLOT : (k + 1) * SLOT] = jnp.concatenate([first, second], axis=1)[:1]


def weight_copies(pieces, wts, w_s, sem, pos):
    x, zh, c = pos[0], pos[1], pos[2]
    moves = []
    for i, (dx, oz, oc) in enumerate(pieces):
        d = ((x + 4 - dx) % 4) * 4 + ((zh + oz) % 2) * 2 + (c + oc) % 2
        dst = w_s.at[pl.ds(aligned(d, HEAD_DIM), HEAD_DIM)]
        moves.append((None, pltpu.make_async_copy(wts[i].at[pl.ds(oz * HEAD_DIM, HEAD_DIM)], dst, sem.at[i])))
    return moves


def head_columns(pos, k):
    return pl.ds(aligned((pos[4] + k) % 4, SLOT), SLOT)


def project_kernel(pieces, pos, own, u1, u2, d1, d2, *refs):
    wts = refs[: len(pieces)]
    gain, shift_by, bias = refs[len(pieces) : len(pieces) + 3]
    outs = refs[len(pieces) + 3 : len(pieces) + 11]
    tok_s, nrm_s, w_s, sem_t, sem_w = refs[len(pieces) + 11 :]
    zl = pos[3]
    rows = own.shape[0]

    def copy_in(src, z, n):
        return pltpu.make_async_copy(src, tok_s.at[pl.ds(aligned(jnp.clip(z, 0, 3), rows), rows)], sem_t.at[n])

    moves = [
        (None, copy_in(own, zl, 0)),
        (zl >= 1, copy_in(u1, zl - 1, 1)),
        (zl >= 2, copy_in(u2, zl - 2, 2)),
        (zl <= 2, copy_in(d1, zl + 1, 3)),
        (zl <= 1, copy_in(d2, zl + 2, 4)),
        ((zl == 0) | (zl == 3), copy_in(own, 3 - zl, 5)),
    ]
    run_copies(moves)
    w_moves = weight_copies(pieces, wts, w_s, sem_w, pos)
    run_copies(w_moves)
    wait_copies(moves)
    normalize_rows(tok_s, nrm_s, gain, shift_by, 96)
    wait_copies(w_moves)
    part = rows // 2

    def two_blocks(n, carry):
        blocks = nrm_s[pl.ds(aligned(n, 2 * rows), 2 * rows)]
        for k in range(4):
            cols = head_columns(pos, k)
            acc = jnp.dot(blocks, w_s[:, cols], preferred_element_type=F32)
            acc = (acc + bias[:, cols]).astype(BF)
            for z in range(2):
                for i in range(2):
                    to = pl.ds(aligned(2 * n + z, part), part)
                    outs[i * 4 + k][to] = acc[z * rows + i * part : z * rows + (i + 1) * part]
        return carry

    lax.fori_loop(0, 2, two_blocks, 0)


def late_kernel(pieces, pos, u3, d3, *refs):
    wts = refs[: len(pieces)]
    gain, shift_by, bias = refs[len(pieces) : len(pieces) + 3]
    outs = refs[len(pieces) + 11 : len(pieces) + 19]
    tok_s, nrm_s, w_s, out_s, sem_t, sem_w, sem_o = refs[len(pieces) + 19 :]
    zl = pos[3]
    rows = u3.shape[0]
    part = rows // 2

    @pl.when((zl == 0) | (zl == 3))
    def _():
        moves = [
            (zl == 3, pltpu.make_async_copy(u3, tok_s, sem_t.at[0])),
            (zl == 0, pltpu.make_async_copy(d3, tok_s, sem_t.at[1])),
        ]
        run_copies(moves)
        w_moves = weight_copies(pieces, wts, w_s, sem_w, pos)
        run_copies(w_moves)
        wait_copies(moves)
        normalize_rows(tok_s, nrm_s, gain, shift_by, 96)
        wait_copies(w_moves)

        def one(k, carry):
            cols = head_columns(pos, k)
            acc = jnp.dot(nrm_s[...], w_s[:, cols], preferred_element_type=F32)
            out_s[k] = (acc + bias[:, cols]).astype(BF)
            return carry

        lax.fori_loop(0, 4, one, 0)
        out_moves = []
        for k in range(4):
            for i in range(2):
                dst = outs[i * 4 + k].at[pl.ds(aligned(3 - zl, part), part)]
                copy = pltpu.make_async_copy(out_s.at[k, pl.ds(i * part, part)], dst, sem_o.at[i * 4 + k])
                out_moves.append((None, copy))
        run_copies(out_moves)
        wait_copies(out_moves)


def attend_kernel(block_rows, pos, b0, b1, b2, b3, out, s_ref, sem):
    y = pos[4]
    rows = b0.shape[0]
    part, third = rows // 4, rows // 12
    copies = [
        (None, pltpu.make_async_copy(b, s_ref.at[pl.ds(k * rows, rows)], sem.at[k]))
        for k, b in enumerate((b0, b1, b2, b3))
    ]
    run_copies(copies)
    wait_copies(copies)
    factor = math.log2(math.e) / math.sqrt(HEAD_DIM)
    lane = lax.broadcasted_iota(jnp.int32, (block_rows, LANES), 1)
    thin = lax.broadcasted_iota(jnp.int32, (third, LANES), 1)

    def one(r, carry):
        at = pl.ds(aligned(r, block_rows), block_rows)
        q = s_ref[at, :LANES]
        q = jnp.where(lane < HEAD_DIM, q, jnp.zeros_like(q))
        scores = lax.dot_general(q, s_ref[:, LANES:], (((1,), (1,)), ((), ())), preferred_element_type=F32)
        highest = jnp.max(scores, axis=-1, keepdims=True)
        weights = jnp.exp2((scores - highest) * factor).astype(BF)
        mixed = jnp.dot(weights, s_ref[...], preferred_element_type=F32)
        total = mixed[:, LANES + USED : LANES + USED + 1]
        first = pltpu.roll(mixed[:, :LANES], LANES - HEAD_DIM, 1)
        second = pltpu.roll(mixed[:, LANES:], LANES - (HEAD_DIM - FIRST), 1)
        joined = jnp.where(lane < FIRST, first, second)
        joined = jnp.where(lane < HEAD_DIM, joined / total, 0.0)
        for p in range(block_rows // part):
            g = r * (block_rows // part) + p
            a, b, c = (joined[p * part + t * third : p * part + (t + 1) * third] for t in range(3))
            b, c = pltpu.roll(b, HEAD_DIM, 1), pltpu.roll(c, 2 * HEAD_DIM - LANES, 1)
            tile0 = jnp.where(thin < HEAD_DIM, a, b)
            tile1 = jnp.where(thin < 2 * HEAD_DIM - LANES, b, c)
            out[(g % 4) * 4 + (y + 4 - g // 4) % 4] = jnp.concatenate([tile0, tile1], axis=1).astype(BF)
        return carry

    lax.fori_loop(0, 4 * rows // block_rows, one, 0, unroll=2)


def spread(block):
    lane = lax.broadcasted_iota(jnp.int32, (block.shape[0], LANES), 1)
    t0, t1 = block[:, :LANES].astype(F32), block[:, LANES:].astype(F32)
    back = LANES - HEAD_DIM
    middle = jnp.where(lane < back, pltpu.roll(t0, back, 1), pltpu.roll(t1, back, 1))
    parts = [t0, middle, pltpu.roll(t1, 2 * LANES - 2 * HEAD_DIM, 1)]
    return jnp.concatenate([jnp.where(lane < HEAD_DIM, p, 0.0) for p in parts], axis=0)


def finish_kernel(own, other, pos, c0, c1, tokens, *refs):
    own_w, other_w = refs[: len(own)], refs[len(own) : len(own) + len(other)]
    out_bias, mlp_gain, mlp_shift, up_bias, down_bias, out = refs[len(own) + len(other) :][:6]
    w_s, ctx_s, mid_s, nrm_s, hid_s, sem = refs[len(own) + len(other) + 6 :]
    x, zh, c, y = pos[0], pos[1], pos[2], pos[4]
    stages = [[], [], []]
    n = 0

    def place(dx, oz, oc):
        return ((x + 4 - dx) % 4) * 4 + ((zh + oz) % 2) * 2 + (c + oc) % 2

    for i, (dx, oc, row0, count) in enumerate(own):
        for stage, (low, high) in enumerate(((0, 1), (1, 3), (3, 5))):
            low, high = low * HEAD_DIM, high * HEAD_DIM
            if row0 <= low and high <= row0 + count:
                src = own_w[i].at[pl.ds(low - row0, high - low)]
                dst = w_s.at[place(dx, 0, oc), pl.ds(low, high - low)]
                stages[stage].append((None, pltpu.make_async_copy(src, dst, sem.at[n])))
                n += 1
    for i, (dx, oc, step0, steps) in enumerate(other):
        for q in range(4):
            k = (y + 4 - q) % 4
            inside = None if steps == 4 else (k >= step0) & (k < step0 + steps)
            at = jnp.clip(k - step0, 0, steps - 1)
            src = other_w[i].at[pl.ds(aligned(at, QUARTER), QUARTER)]
            dst = w_s.at[place(dx, 1, oc), pl.ds(q * QUARTER, QUARTER)]
            stages[(0, 1, 1, 2)[q]].append((inside, pltpu.make_async_copy(src, dst, sem.at[n])))
            n += 1
    for group in stages:
        run_copies(group)
    rows, width = tokens.shape[1], tokens.shape[2]
    lane = lax.broadcasted_iota(jnp.int32, (rows, LANES), 1)
    for i, ctx in enumerate((c0, c1)):
        tiles = [None] * (width // LANES)
        for h in range(HEADS):
            t, off = divmod(h * HEAD_DIM, LANES)
            moved = spread(ctx[h])
            if off == 0:
                tiles[t] = moved
                continue
            moved = pltpu.roll(moved, off, 1)
            tiles[t] = jnp.where(lane >= off, moved, tiles[t])
            if off + HEAD_DIM > LANES:
                tiles[t + 1] = moved
        for t, tile in enumerate(tiles):
            ctx_s[i * rows : (i + 1) * rows, t * LANES : (t + 1) * LANES] = tile.astype(BF)
    wait_copies(stages[0])

    def project_out(n, carry):
        cols = pl.ds(aligned(n, SLOT), SLOT)
        w = w_s[:, :HEAD_DIM, cols].reshape(width, SLOT)
        attended = jnp.dot(ctx_s[...], w, preferred_element_type=F32) + out_bias[cols].reshape(1, SLOT)
        for i in range(2):
            at = slice(i * rows, (i + 1) * rows)
            mid_s[at, cols] = tokens[i, :, cols].astype(F32) + attended[at]
        return carry

    lax.fori_loop(0, width // SLOT, project_out, 0)
    normalize_rows(mid_s, nrm_s, mlp_gain, mlp_shift, 96)
    wait_copies(stages[1])

    def lift(n, carry):
        for half in range(2):
            cols = pl.ds(aligned(n, SLOT), SLOT)
            to = pl.ds(aligned(n + half * (width // SLOT), SLOT), SLOT)
            w = w_s[:, HEAD_DIM * (1 + half) : HEAD_DIM * (2 + half), cols].reshape(width, SLOT)
            lifted = jnp.dot(nrm_s[...], w, preferred_element_type=F32) + up_bias[to].reshape(1, SLOT)
            hid_s[:, to] = (0.5 * lifted * (1.0 + lax.erf(lifted * math.sqrt(0.5)))).astype(BF)
        return carry

    lax.fori_loop(0, width // SLOT, lift, 0)
    wait_copies(stages[2])

    def lower(n, carry):
        cols = pl.ds(aligned(n, SLOT), SLOT)
        w = w_s[:, HEAD_DIM * 3 : HEAD_DIM * 5, cols].reshape(2 * width, SLOT)
        lowered = jnp.dot(hid_s[...], w, preferred_element_type=F32)
        result = (mid_s[:, cols] + lowered + down_bias[cols].reshape(1, SLOT)).astype(BF)
        for i in range(2):
            out[i, :, cols] = result[i * rows : (i + 1) * rows]
        return carry

    lax.fori_loop(0, width // SLOT, lower, 0)


def ring_gather(a):
    for dx in range(4):
        b = a if dx == 0 else shift(a, "x", dx, 4)
        across = swap_core(b)
        yield dx, 0, b
        yield dx, 1, across


def swap_core(a):
    return lax.ppermute(a, "c", [(0, 1), (1, 0)])


def swap_half(a):
    return lax.ppermute(a, "zh", [(0, 1), (1, 0)])


def ring_z(a, by):
    return lax.ppermute(a, ("zh", "zl"), [(i, (i + by) % 8) for i in range(8)])


def shards(tokens, pre_gain, pre_shift, w_qkv, qkv_bias, w_out, out_bias, mlp_gain, mlp_shift, w_up, up_bias, w_down, down_bias):
    images, tok_here, width = tokens.shape
    pos = jnp.stack([lax.axis_index(n) for n in ("x", "zh", "c", "zl", "y")]).astype(jnp.int32)

    ups, downs = [tokens.reshape(images * tok_here, width)], [tokens.reshape(images * tok_here, width)]
    for _ in range(3):
        ups.append(ring_z(ups[-1], 1))
        downs.append(ring_z(downs[-1], -1))

    slots, bias, pack, quarter = pl.pallas_call(
        prepare_kernel,
        out_shape=[
            jax.ShapeDtypeStruct((HEAD_DIM, 4 * SLOT), BF),
            jax.ShapeDtypeStruct((1, 4 * SLOT), F32),
            jax.ShapeDtypeStruct((5 * HEAD_DIM, width), BF),
            jax.ShapeDtypeStruct((QUARTER, width), BF),
        ],
        in_specs=[SMEM] + [VMEM] * 5,
        out_specs=[VMEM] * 4,
        scratch_shapes=[pltpu.VMEM((4 * QUARTER, width), BF)],
        name="prepare",
    )(pos, w_qkv, qkv_bias.reshape(1, -1), w_out, w_up, w_down)
    got = swap_half(slots)
    quarters = [swap_half(quarter)]

    both = jnp.concatenate([slots, got], axis=0)
    wq_pieces, wq_arrays = [], []
    for dx in range(4):
        a = both if dx == 0 else shift(both, "x", dx, 4)
        across = swap_core(a)
        for oc, b in ((0, a), (1, across)):
            for oz in range(2):
                wq_pieces.append((dx, oz, oc))
                wq_arrays.append(b)

    for k in (1, 2, 3):
        quarters.append(shift(quarters[0], "y", k, 4))
    joined = jax.ShapeDtypeStruct((4 * QUARTER, width), BF)
    quarters = pl.pallas_call(join_kernel, out_shape=joined, in_specs=[VMEM] * 4, out_specs=VMEM, name="join")(*quarters)
    own, own_arrays, other, other_arrays = [], [], [], []
    for dx, oc, a in ring_gather(pack):
        own.append((dx, oc, 0, a.shape[0]))
        own_arrays.append(a)
    for dx, oc, a in ring_gather(quarters):
        other.append((dx, oc, 0, 4))
        other_arrays.append(a)

    rows = images * tok_here
    n_wq = len(wq_arrays)
    half = jax.ShapeDtypeStruct((4 * tok_here, SLOT), BF)
    project = pl.pallas_call(
        lambda *refs: project_kernel(tuple(wq_pieces), *refs),
        out_shape=[half] * 8,
        in_specs=[SMEM] + [ANY] * (5 + n_wq) + [VMEM] * 3,
        out_specs=[VMEM] * 8,
        scratch_shapes=[
            pltpu.VMEM((4 * rows, width), BF),
            pltpu.VMEM((4 * rows, width), BF),
            pltpu.VMEM((width, 4 * SLOT), BF),
            pltpu.SemaphoreType.DMA((6,)),
            pltpu.SemaphoreType.DMA((n_wq,)),
        ],
        name="project",
        cost_estimate=pl.CostEstimate(flops=2 * 1152 * 1280 * 1024, bytes_accessed=9000000, transcendentals=0),
    )
    late = pl.pallas_call(
        lambda *refs: late_kernel(tuple(wq_pieces), *refs),
        out_shape=[half] * 8,
        in_specs=[SMEM] + [ANY] * (2 + n_wq) + [VMEM] * 3 + [ANY] * 8,
        out_specs=[ANY] * 8,
        input_output_aliases={6 + n_wq + i: i for i in range(8)},
        scratch_shapes=[
            pltpu.VMEM((rows, width), BF),
            pltpu.VMEM((rows, width), BF),
            pltpu.VMEM((width, 4 * SLOT), BF),
            pltpu.VMEM((4, rows, SLOT), BF),
            pltpu.SemaphoreType.DMA((2,)),
            pltpu.SemaphoreType.DMA((n_wq,)),
            pltpu.SemaphoreType.DMA((8,)),
        ],
        name="late",
        cost_estimate=pl.CostEstimate(flops=2 * 288 * 1280 * 1024, bytes_accessed=4000000, transcendentals=0),
    )
    early = project(pos, ups[0], ups[1], ups[2], downs[1], downs[2], *wq_arrays, pre_gain, pre_shift, bias)
    packed = late(pos, ups[3], downs[3], *wq_arrays, pre_gain, pre_shift, bias, *early)

    contexts = []
    for i in range(images):
        attend = pl.pallas_call(
            lambda *refs: attend_kernel(288, *refs),
            out_shape=jax.ShapeDtypeStruct((HEADS, tok_here // 3, SLOT), BF),
            in_specs=[SMEM] + [ANY] * 4,
            out_specs=VMEM,
            scratch_shapes=[pltpu.VMEM((HEADS * tok_here, SLOT), BF), pltpu.SemaphoreType.DMA((4,))],
            name="attend",
            cost_estimate=pl.CostEstimate(flops=4 * 2304 * 2304 * 256, bytes_accessed=2000000, transcendentals=2304 * 2304),
        )
        four = [packed[i * 4]]
        for k in (1, 2, 3):
            four.append(shift(packed[i * 4 + k], "y", k, 4))
        ctx = attend(pos, *four)
        contexts.append(lax.all_to_all(ctx, ("zl", "y"), split_axis=0, concat_axis=0, tiled=True))

    n_copies = 3 * len(own) + 4 * len(other)
    return pl.pallas_call(
        lambda *refs: finish_kernel(tuple(own), tuple(other), *refs),
        out_shape=jax.ShapeDtypeStruct(tokens.shape, BF),
        in_specs=[SMEM, VMEM, VMEM, VMEM] + [ANY] * (len(own) + len(other)) + [VMEM] * 5,
        out_specs=VMEM,
        scratch_shapes=[
            pltpu.VMEM((HEADS, 4 * QUARTER, width), BF),
            pltpu.VMEM((images * tok_here, width), BF),
            pltpu.VMEM((images * tok_here, width), F32),
            pltpu.VMEM((images * tok_here, width), BF),
            pltpu.VMEM((images * tok_here, 2 * width), BF),
            pltpu.SemaphoreType.DMA((n_copies,)),
        ],
        name="finish",
        cost_estimate=pl.CostEstimate(flops=4700000000, bytes_accessed=20000000, transcendentals=288 * 2560),
    )(pos, *contexts, tokens, *own_arrays, *other_arrays, out_bias, mlp_gain, mlp_shift, up_bias, down_bias)


def solution(mesh):
    dp, seq = ("x", "zh", "c"), ("zl", "y")
    fine = Mesh(mesh.devices.reshape(4, 2, 2, 4, 4), dp + seq)
    rows = P(dp, None)
    in_specs = (P(dp, seq, None), P(), P(), rows, P(), rows, P(), P(), P(), rows, P(), rows, P())
    return jax.shard_map(shards, mesh=fine, in_specs=in_specs, out_specs=P(dp, seq, None), check_vma=False)
```

```python
import math

import jax
import jax.numpy as jnp
from jax import lax
from jax.experimental import pallas as pl
from jax.experimental.pallas import tpu as pltpu
from jax.sharding import Mesh
from jax.sharding import PartitionSpec as P


HEADS = 16
HEAD_DIM = 80
EPSILON = 1e-05
LANES = 128
SLOT = 2 * LANES
FIRST = LANES - HEAD_DIM
QUARTER = 112
USED = 112
BF = jnp.bfloat16
F32 = jnp.float32
ANY = pl.BlockSpec(memory_space=pltpu.HBM)
SMEM = pl.BlockSpec(memory_space=pltpu.SMEM)
VMEM = pl.BlockSpec(memory_space=pltpu.VMEM)


def shift(a, axis, by, size):
    return lax.ppermute(a, axis, [(i, (i + by) % size) for i in range(size)])


def normalize(features, gain, shift_by):
    average = jnp.mean(features, axis=-1, keepdims=True)
    centered = features - average
    spread = jnp.mean(centered * centered, axis=-1, keepdims=True)
    return centered * lax.rsqrt(spread + EPSILON) * gain + shift_by


def normalize_rows(src, dst, gain, shift_by, step):
    def some(n, carry):
        at = pl.ds(aligned(n, step), step)
        dst[at] = normalize(src[at].astype(F32), line(gain), line(shift_by)).astype(BF)
        return carry

    lax.fori_loop(0, src.shape[0] // step, some, 0)


def join_kernel(*refs):
    parts, outs = refs[:-2], refs[-2:]
    for i, part in enumerate(parts):
        at = i % 2 * QUARTER
        outs[i // 2][at : at + QUARTER] = part[...]


def run_copies(copies):
    for when, copy in copies:
        if when is None:
            copy.start()
        else:
            pl.when(when)(copy.start)


def wait_copies(copies):
    for when, copy in copies:
        if when is None:
            copy.wait()
        else:
            pl.when(when)(copy.wait)


def line(v, start=0, size=None):
    size = v.shape[0] if size is None else size
    return v[start : start + size].reshape(1, size)


def aligned(i, m):
    return pl.multiple_of(i * m, m)


def prepare_kernel(pos, w_qkv, qkv_bias, w_out, w_up, w_down, slots, bias, pack, quarter, pad_s):
    zl, y = pos[3], pos[4]
    width = pack.shape[1]
    pad_s[: HEAD_DIM] = w_out[...]
    pad_s[HEAD_DIM : 2 * HEAD_DIM] = w_up[:, :width]
    pad_s[2 * HEAD_DIM : 3 * HEAD_DIM] = w_up[:, width:]
    pad_s[3 * HEAD_DIM : 5 * HEAD_DIM] = w_down[...]
    pad_s[5 * HEAD_DIM :] = jnp.zeros((4 * QUARTER - 5 * HEAD_DIM, width), BF)
    pack[...] = pad_s[: 5 * HEAD_DIM]
    quarter[...] = pad_s[pl.ds(aligned(y, QUARTER), QUARTER)]

    def two_tiles(window):
        lane = lax.broadcasted_iota(jnp.int32, (window.shape[0], LANES), 1)
        ahead = pltpu.roll(window, 3 * LANES - HEAD_DIM, 1)[:, :LANES]
        first = jnp.where(lane < HEAD_DIM, window[:, :LANES], ahead)
        second = jnp.where(lane < HEAD_DIM, ahead, window[:, LANES:SLOT])
        return first, second, lane

    for k in range(4):
        first_column = (4 * zl + k) * 3 * HEAD_DIM
        start = jnp.minimum(first_column // LANES, w_qkv.shape[1] // LANES - 3)
        turn = (3 * LANES - (first_column - start * LANES)) % (3 * LANES)
        cols = pl.ds(aligned(start, LANES), 3 * LANES)
        w = pltpu.roll(w_qkv[:, cols].astype(F32), turn, 1)
        v = pltpu.roll(jnp.broadcast_to(qkv_bias[:, cols], (8, 3 * LANES)), turn, 1)
        first, second, lane = two_tiles(w)
        both = jnp.concatenate([first, jnp.where(lane < USED, second, 0.0)], axis=1)
        slots[:, k * SLOT : (k + 1) * SLOT] = both.astype(BF)
        first, second, lane = two_tiles(v)
        second = jnp.where(lane < USED, second, jnp.where(lane == USED, 1.0, 0.0))
        bias[:, k * SLOT : (k + 1) * SLOT] = jnp.concatenate([first, second], axis=1)[:1]


def weight_copies(pieces, wts, w_s, sem, pos):
    x, zh, c = pos[0], pos[1], pos[2]
    moves = []
    for i, (dx, oz, oc) in enumerate(pieces):
        d = ((x + 4 - dx) % 4) * 4 + ((zh + oz) % 2) * 2 + (c + oc) % 2
        dst = w_s.at[pl.ds(aligned(d, HEAD_DIM), HEAD_DIM)]
        moves.append((None, pltpu.make_async_copy(wts[i].at[pl.ds(oz * HEAD_DIM, HEAD_DIM)], dst, sem.at[i])))
    return moves


def head_columns(pos, k):
    return pl.ds(aligned((pos[4] + k) % 4, SLOT), SLOT)


def project_kernel(pieces, pos, own, u1, u2, d1, d2, *refs):
    wts = refs[: len(pieces)]
    gain, shift_by, bias = refs[len(pieces) : len(pieces) + 3]
    outs = refs[len(pieces) + 3 : len(pieces) + 11]
    tok_s, nrm_s, w_s, sem_t, sem_w = refs[len(pieces) + 11 :]
    zl = pos[3]
    rows = own.shape[0]

    def copy_in(src, z, n):
        return pltpu.make_async_copy(src, tok_s.at[pl.ds(aligned(jnp.clip(z, 0, 3), rows), rows)], sem_t.at[n])

    moves = [
        (None, copy_in(own, zl, 0)),
        (zl >= 1, copy_in(u1, zl - 1, 1)),
        (zl >= 2, copy_in(u2, zl - 2, 2)),
        (zl <= 2, copy_in(d1, zl + 1, 3)),
        (zl <= 1, copy_in(d2, zl + 2, 4)),
        ((zl == 0) | (zl == 3), copy_in(own, 3 - zl, 5)),
    ]
    run_copies(moves)
    w_moves = weight_copies(pieces, wts, w_s, sem_w, pos)
    run_copies(w_moves)
    wait_copies(moves)
    nrm_s[...] = normalize(tok_s[...].astype(F32), line(gain), line(shift_by)).astype(BF)
    wait_copies(w_moves)
    part = rows // 2
    for k in range(4):
        cols = head_columns(pos, k)
        acc = jnp.dot(nrm_s[...], w_s[:, cols], preferred_element_type=F32)
        acc = (acc + bias[:, cols]).astype(BF)
        for z in range(4):
            for i in range(2):
                outs[i * 4 + k][z * part : (z + 1) * part] = acc[z * rows + i * part : z * rows + (i + 1) * part]


def late_kernel(pieces, pos, u3, d3, *refs):
    wts = refs[: len(pieces)]
    gain, shift_by, bias = refs[len(pieces) : len(pieces) + 3]
    outs = refs[len(pieces) + 11 : len(pieces) + 19]
    tok_s, nrm_s, w_s, out_s, sem_t, sem_w, sem_o = refs[len(pieces) + 19 :]
    zl = pos[3]
    rows = u3.shape[0]
    part = rows // 2

    @pl.when((zl == 0) | (zl == 3))
    def _():
        moves = [
            (zl == 3, pltpu.make_async_copy(u3, tok_s, sem_t.at[0])),
            (zl == 0, pltpu.make_async_copy(d3, tok_s, sem_t.at[1])),
        ]
        run_copies(moves)
        w_moves = weight_copies(pieces, wts, w_s, sem_w, pos)
        run_copies(w_moves)
        wait_copies(moves)
        nrm_s[...] = normalize(tok_s[...].astype(F32), line(gain), line(shift_by)).astype(BF)
        wait_copies(w_moves)
        out_moves = []
        for k in range(4):
            cols = head_columns(pos, k)
            acc = jnp.dot(nrm_s[...], w_s[:, cols], preferred_element_type=F32)
            out_s[k] = (acc + bias[:, cols]).astype(BF)
            for i in range(2):
                dst = outs[i * 4 + k].at[pl.ds(aligned(3 - zl, part), part)]
                copy = pltpu.make_async_copy(out_s.at[k, pl.ds(i * part, part)], dst, sem_o.at[i * 4 + k])
                out_moves.append((None, copy))
            run_copies(out_moves[-2:])
        wait_copies(out_moves)


def attend_kernel(block_rows, pos, b0, b1, b2, b3, out, s_ref, sem):
    y = pos[4]
    rows = b0.shape[0]
    part, third = rows // 4, rows // 12
    copies = [
        (None, pltpu.make_async_copy(b, s_ref.at[pl.ds(k * rows, rows)], sem.at[k]))
        for k, b in enumerate((b0, b1, b2, b3))
    ]
    run_copies(copies)
    wait_copies(copies)
    factor = math.log2(math.e) / math.sqrt(HEAD_DIM)
    lane = lax.broadcasted_iota(jnp.int32, (block_rows, LANES), 1)
    thin = lax.broadcasted_iota(jnp.int32, (third, LANES), 1)

    def one(r, carry):
        at = pl.ds(aligned(r, block_rows), block_rows)
        q = s_ref[at, :LANES]
        q = jnp.where(lane < HEAD_DIM, q, jnp.zeros_like(q))
        scores = lax.dot_general(q, s_ref[:, LANES:], (((1,), (1,)), ((), ())), preferred_element_type=F32)
        highest = jnp.max(scores, axis=-1, keepdims=True)
        weights = jnp.exp2((scores - highest) * factor).astype(BF)
        mixed = jnp.dot(weights, s_ref[...], preferred_element_type=F32)
        total = mixed[:, LANES + USED : LANES + USED + 1]
        first = pltpu.roll(mixed[:, :LANES], LANES - HEAD_DIM, 1)
        second = pltpu.roll(mixed[:, LANES:], LANES - (HEAD_DIM - FIRST), 1)
        joined = jnp.where(lane < FIRST, first, second)
        joined = jnp.where(lane < HEAD_DIM, joined / total, 0.0)
        for p in range(block_rows // part):
            g = r * (block_rows // part) + p
            a, b, c = (joined[p * part + t * third : p * part + (t + 1) * third] for t in range(3))
            b, c = pltpu.roll(b, HEAD_DIM, 1), pltpu.roll(c, 2 * HEAD_DIM - LANES, 1)
            tile0 = jnp.where(thin < HEAD_DIM, a, b)
            tile1 = jnp.where(thin < 2 * HEAD_DIM - LANES, b, c)
            out[(g % 4) * 4 + (y + 4 - g // 4) % 4] = jnp.concatenate([tile0, tile1], axis=1).astype(BF)
        return carry

    lax.fori_loop(0, 4 * rows // block_rows, one, 0, unroll=True)


def spread(block):
    lane = lax.broadcasted_iota(jnp.int32, (block.shape[0], LANES), 1)
    t0, t1 = block[:, :LANES].astype(F32), block[:, LANES:].astype(F32)
    back = LANES - HEAD_DIM
    middle = jnp.where(lane < back, pltpu.roll(t0, back, 1), pltpu.roll(t1, back, 1))
    parts = [t0, middle, pltpu.roll(t1, 2 * LANES - 2 * HEAD_DIM, 1)]
    return jnp.concatenate([jnp.where(lane < HEAD_DIM, p, 0.0) for p in parts], axis=0)


def finish_kernel(own, other, pos, c0, c1, tokens, *refs):
    own_w, other_w = refs[: len(own)], refs[len(own) : len(own) + len(other)]
    out_bias, mlp_gain, mlp_shift, up_bias, down_bias, out = refs[len(own) + len(other) :][:6]
    w_s, ctx_s, mid_s, nrm_s, hid_s, sem = refs[len(own) + len(other) + 6 :]
    x, zh, c, y = pos[0], pos[1], pos[2], pos[4]
    stages = [[], [], []]
    n = 0

    def place(dx, oz, oc):
        return ((x + 4 - dx) % 4) * 4 + ((zh + oz) % 2) * 2 + (c + oc) % 2

    for i, (dx, oc, row0, count) in enumerate(own):
        for stage, (low, high) in enumerate(((0, 1), (1, 3), (3, 5))):
            low, high = low * HEAD_DIM, high * HEAD_DIM
            if row0 <= low and high <= row0 + count:
                src = own_w[i].at[pl.ds(low - row0, high - low)]
                dst = w_s.at[place(dx, 0, oc), pl.ds(low, high - low)]
                stages[stage].append((None, pltpu.make_async_copy(src, dst, sem.at[n])))
                n += 1
    for i, (dx, oc, step0, steps) in enumerate(other):
        for q in range(4):
            k = (y + 4 - q) % 4
            inside = None if steps == 4 else (k >= step0) & (k < step0 + steps)
            at = jnp.clip(k - step0, 0, steps - 1)
            src = other_w[i].at[pl.ds(aligned(at, QUARTER), QUARTER)]
            dst = w_s.at[place(dx, 1, oc), pl.ds(q * QUARTER, QUARTER)]
            stages[(0, 1, 1, 2)[q]].append((inside, pltpu.make_async_copy(src, dst, sem.at[n])))
            n += 1
    for group in stages:
        run_copies(group)
    rows, width = tokens.shape[1], tokens.shape[2]
    lane = lax.broadcasted_iota(jnp.int32, (rows, LANES), 1)
    for i, ctx in enumerate((c0, c1)):
        tiles = [None] * (width // LANES)
        for h in range(HEADS):
            t, off = divmod(h * HEAD_DIM, LANES)
            moved = spread(ctx[h])
            if off == 0:
                tiles[t] = moved
                continue
            moved = pltpu.roll(moved, off, 1)
            tiles[t] = jnp.where(lane >= off, moved, tiles[t])
            if off + HEAD_DIM > LANES:
                tiles[t + 1] = moved
        for t, tile in enumerate(tiles):
            ctx_s[i * rows : (i + 1) * rows, t * LANES : (t + 1) * LANES] = tile.astype(BF)
    wait_copies(stages[0])

    def project_out(n, carry):
        cols = pl.ds(aligned(n, SLOT), SLOT)
        w = w_s[:, :HEAD_DIM, cols].reshape(width, SLOT)
        attended = jnp.dot(ctx_s[...], w, preferred_element_type=F32) + out_bias[cols].reshape(1, SLOT)
        for i in range(2):
            at = slice(i * rows, (i + 1) * rows)
            mid_s[at, cols] = tokens[i, :, cols].astype(F32) + attended[at]
        return carry

    lax.fori_loop(0, width // SLOT, project_out, 0, unroll=True)
    normalize_rows(mid_s, nrm_s, mlp_gain, mlp_shift, 96)
    wait_copies(stages[1])

    def lift(n, carry):
        for half in range(2):
            cols = pl.ds(aligned(n, SLOT), SLOT)
            to = pl.ds(aligned(n + half * (width // SLOT), SLOT), SLOT)
            w = w_s[:, HEAD_DIM * (1 + half) : HEAD_DIM * (2 + half), cols].reshape(width, SLOT)
            lifted = jnp.dot(nrm_s[...], w, preferred_element_type=F32) + up_bias[to].reshape(1, SLOT)
            hid_s[:, to] = (0.5 * lifted * (1.0 + lax.erf(lifted * math.sqrt(0.5)))).astype(BF)
        return carry

    lax.fori_loop(0, width // SLOT, lift, 0, unroll=True)
    wait_copies(stages[2])

    def lower(n, carry):
        cols = pl.ds(aligned(n, SLOT), SLOT)
        w = w_s[:, HEAD_DIM * 3 : HEAD_DIM * 5, cols].reshape(2 * width, SLOT)
        lowered = jnp.dot(hid_s[...], w, preferred_element_type=F32)
        result = (mid_s[:, cols] + lowered + down_bias[cols].reshape(1, SLOT)).astype(BF)
        for i in range(2):
            out[i, :, cols] = result[i * rows : (i + 1) * rows]
        return carry

    lax.fori_loop(0, width // SLOT, lower, 0, unroll=True)


def ring_gather(a):
    for dx in range(4):
        b = a if dx == 0 else shift(a, "x", dx, 4)
        across = swap_core(b)
        yield dx, 0, b
        yield dx, 1, across


def swap_core(a):
    return lax.ppermute(a, "c", [(0, 1), (1, 0)])


def swap_half(a):
    return lax.ppermute(a, "zh", [(0, 1), (1, 0)])


def ring_z(a, by):
    return lax.ppermute(a, ("zh", "zl"), [(i, (i + by) % 8) for i in range(8)])


def shards(tokens, pre_gain, pre_shift, w_qkv, qkv_bias, w_out, out_bias, mlp_gain, mlp_shift, w_up, up_bias, w_down, down_bias):
    images, tok_here, width = tokens.shape
    pos = jnp.stack([lax.axis_index(n) for n in ("x", "zh", "c", "zl", "y")]).astype(jnp.int32)

    ups, downs = [tokens.reshape(images * tok_here, width)], [tokens.reshape(images * tok_here, width)]
    for _ in range(3):
        ups.append(ring_z(ups[-1], 1))
        downs.append(ring_z(downs[-1], -1))

    slots, bias, pack, quarter = pl.pallas_call(
        prepare_kernel,
        out_shape=[
            jax.ShapeDtypeStruct((HEAD_DIM, 4 * SLOT), BF),
            jax.ShapeDtypeStruct((1, 4 * SLOT), F32),
            jax.ShapeDtypeStruct((5 * HEAD_DIM, width), BF),
            jax.ShapeDtypeStruct((QUARTER, width), BF),
        ],
        in_specs=[SMEM] + [VMEM] * 5,
        out_specs=[VMEM] * 4,
        scratch_shapes=[pltpu.VMEM((4 * QUARTER, width), BF)],
        name="prepare",
    )(pos, w_qkv, qkv_bias.reshape(1, -1), w_out, w_up, w_down)
    got = swap_half(slots)
    quarters = [swap_half(quarter)]

    both = jnp.concatenate([slots, got], axis=0)
    wq_pieces, wq_arrays = [], []
    for dx in range(4):
        a = both if dx == 0 else shift(both, "x", dx, 4)
        across = swap_core(a)
        for oc, b in ((0, a), (1, across)):
            for oz in range(2):
                wq_pieces.append((dx, oz, oc))
                wq_arrays.append(b)

    for k in (1, 2, 3):
        quarters.append(shift(quarters[0], "y", k, 4))
    pair = jax.ShapeDtypeStruct((2 * QUARTER, width), BF)
    pairs = pl.pallas_call(join_kernel, out_shape=[pair] * 2, in_specs=[VMEM] * 4, out_specs=[VMEM] * 2, name="join")(*quarters)
    own, own_arrays, other, other_arrays = [], [], [], []
    for dx, oc, a in ring_gather(pack):
        own.append((dx, oc, 0, a.shape[0]))
        own_arrays.append(a)
    hops = {}
    for tag, by in (("a", 1), ("b", 1), ("a", -1), ("b", -1)):
        hops[tag, by] = shift(pairs["ab".index(tag)], "x", by, 4)
    for tag, by in (("a", 1), ("b", -1)):
        hops[tag, 2 * by] = shift(hops[tag, by], "x", by, 4)
    hops["a", 0], hops["b", 0] = pairs
    for (tag, by), a in hops.items():
        across = swap_core(a)
        for oc, b in ((0, a), (1, across)):
            other.append((by % 4, oc, "ab".index(tag) * 2, 2))
            other_arrays.append(b)

    rows = images * tok_here
    n_wq = len(wq_arrays)
    half = jax.ShapeDtypeStruct((4 * tok_here, SLOT), BF)
    project = pl.pallas_call(
        lambda *refs: project_kernel(tuple(wq_pieces), *refs),
        out_shape=[half] * 8,
        in_specs=[SMEM] + [ANY] * (5 + n_wq) + [VMEM] * 3,
        out_specs=[VMEM] * 8,
        scratch_shapes=[
            pltpu.VMEM((4 * rows, width), BF),
            pltpu.VMEM((4 * rows, width), BF),
            pltpu.VMEM((width, 4 * SLOT), BF),
            pltpu.SemaphoreType.DMA((6,)),
            pltpu.SemaphoreType.DMA((n_wq,)),
        ],
        name="project",
        cost_estimate=pl.CostEstimate(flops=2 * 1152 * 1280 * 1024, bytes_accessed=9000000, transcendentals=0),
    )
    late = pl.pallas_call(
        lambda *refs: late_kernel(tuple(wq_pieces), *refs),
        out_shape=[half] * 8,
        in_specs=[SMEM] + [ANY] * (2 + n_wq) + [VMEM] * 3 + [ANY] * 8,
        out_specs=[ANY] * 8,
        input_output_aliases={6 + n_wq + i: i for i in range(8)},
        scratch_shapes=[
            pltpu.VMEM((rows, width), BF),
            pltpu.VMEM((rows, width), BF),
            pltpu.VMEM((width, 4 * SLOT), BF),
            pltpu.VMEM((4, rows, SLOT), BF),
            pltpu.SemaphoreType.DMA((2,)),
            pltpu.SemaphoreType.DMA((n_wq,)),
            pltpu.SemaphoreType.DMA((8,)),
        ],
        name="late",
        cost_estimate=pl.CostEstimate(flops=2 * 288 * 1280 * 1024, bytes_accessed=4000000, transcendentals=0),
    )
    early = project(pos, ups[0], ups[1], ups[2], downs[1], downs[2], *wq_arrays, pre_gain, pre_shift, bias)
    packed = late(pos, ups[3], downs[3], *wq_arrays, pre_gain, pre_shift, bias, *early)

    contexts = []
    for i in range(images):
        attend = pl.pallas_call(
            lambda *refs: attend_kernel(288, *refs),
            out_shape=jax.ShapeDtypeStruct((HEADS, tok_here // 3, SLOT), BF),
            in_specs=[SMEM] + [ANY] * 4,
            out_specs=VMEM,
            scratch_shapes=[pltpu.VMEM((HEADS * tok_here, SLOT), BF), pltpu.SemaphoreType.DMA((4,))],
            cost_estimate=pl.CostEstimate(flops=4 * 2304 * 2304 * 256, bytes_accessed=2000000, transcendentals=2304 * 2304),
        )
        four = [packed[i * 4]]
        for k in (1, 2, 3):
            four.append(shift(packed[i * 4 + k], "y", k, 4))
        ctx = attend(pos, *four)
        contexts.append(lax.all_to_all(ctx, ("zl", "y"), split_axis=0, concat_axis=0, tiled=True))

    n_copies = 3 * len(own) + 4 * len(other)
    return pl.pallas_call(
        lambda *refs: finish_kernel(tuple(own), tuple(other), *refs),
        out_shape=jax.ShapeDtypeStruct(tokens.shape, BF),
        in_specs=[SMEM, VMEM, VMEM, VMEM] + [ANY] * (len(own) + len(other)) + [VMEM] * 5,
        out_specs=VMEM,
        scratch_shapes=[
            pltpu.VMEM((HEADS, 4 * QUARTER, width), BF),
            pltpu.VMEM((images * tok_here, width), BF),
            pltpu.VMEM((images * tok_here, width), F32),
            pltpu.VMEM((images * tok_here, width), BF),
            pltpu.VMEM((images * tok_here, 2 * width), BF),
            pltpu.SemaphoreType.DMA((n_copies,)),
        ],
        name="finish",
        cost_estimate=pl.CostEstimate(flops=4700000000, bytes_accessed=20000000, transcendentals=288 * 2560),
    )(pos, *contexts, tokens, *own_arrays, *other_arrays, out_bias, mlp_gain, mlp_shift, up_bias, down_bias)


def solution(mesh):
    dp, seq = ("x", "zh", "c"), ("zl", "y")
    fine = Mesh(mesh.devices.reshape(4, 2, 2, 4, 4), dp + seq)
    rows = P(dp, None)
    in_specs = (P(dp, seq, None), P(), P(), rows, P(), rows, P(), P(), P(), rows, P(), rows, P())
    return jax.shard_map(shards, mesh=fine, in_specs=in_specs, out_specs=P(dp, seq, None), check_vma=False)
```
